32 devices in a mesh: grp: 8 (over z, core), blk: 4 (over y, x).
Axes of the slice: x: 2, y: 2, z: 4, core: 2. Of those that a mesh axis runs over, the one named last changes fastest.
Arguments:
- integrals: bfloat16 [8, 128, 128, 128], P(None, 'blk'), may hold values from -0.5 to 0.5
- doubles: bfloat16 [64, 128, 128], P('blk'), may hold values from -0.0059814453 to 0.0059814453
- coulomb: bfloat16 [64, 128, 128], P('blk'), may hold values from -0.1796875 to 0.1796875
- singles: float32 [8, 128], P(None, 'blk'), may hold values from -0.18 to 0.18
- occ_energy: float32 [8], replicated, may hold values from -2 to -0.5
- vir_energy: float32 [128], replicated, may hold values from 0.3 to 3
- triplets: int32 [8, 16, 3], P('grp'), may hold values from 0 to 7
- tile_count: int32 [8], P('grp'), may hold values from 1 to 16, as said below
Outputs:
- triplet_energy: float32 [8, 16], P('grp')
- mean_energy: float32 [], replicated
The draws below stay inside these ranges and needn't reach their ends.
Inputs may be any that keep to these rules, and one draw needn't show every extreme that they name: `tile_count`: slots with an index below a group's count are live; some group has all 16 slots live.
All inputs are finite; a program needn't handle non-finite values.
Results may differ from the reference program's by a relative error of at most 0.0003.
Values may be sent and summed in bfloat16 or wider, within the bound.
A program may use at most 64 MiB of HBM per device.

```python
import jax
import jax.numpy as jnp
from jax import lax

NO = 8
NV = 128
TRIP = 16
GROUPS = 8


def draw_tile_count(key, part):
    key_counts = jax.random.fold_in(key, 11)
    key_full = jax.random.fold_in(key, 12)
    counts = jax.random.randint(key_counts, (GROUPS,), max(1, TRIP // 4), TRIP + 1)
    fullest = jax.random.randint(key_full, (), 0, GROUPS)
    return jnp.where(jnp.arange(GROUPS) == fullest, TRIP, counts).astype(jnp.int32)


def with_ends(drawn, rng, least, top_value):
    place = [jax.random.randint(jax.random.fold_in(rng, axis), (), 0, length) for axis, length in enumerate(drawn.shape)]
    main_axis = drawn.shape.index(max(drawn.shape))
    beside = place[:main_axis] + [(place[main_axis] + 1) % drawn.shape[main_axis]] + place[main_axis + 1:]
    return drawn.at[tuple(place)].set(least).at[tuple(beside)].set(top_value)


def level_of(stream_key, extent, split, smallest, high):
    factor_of = 1.0
    for dim, shards_of in split:
        draws = jax.random.uniform(jax.random.fold_in(jax.random.fold_in(stream_key, 6), dim), (shards_of,), jnp.float32, smallest / len(split), high / len(split))
        factor_of = factor_of * jnp.repeat(jnp.exp(draws), extent[dim] // shards_of).reshape((-1,) + (1,) * (len(extent) - 1 - dim))
    return factor_of


def gaussian(own_key, shape, deviation, bound, split=(), kind=jnp.bfloat16):
    entries = jax.random.normal(own_key, shape, jnp.float32) * deviation
    if len(split) > 0:
        entries = level_of(own_key, shape, split, -0.22, 0.18) * entries
    return jnp.clip(entries, min=-bound, max=bound).astype(kind)


def setup_inputs(seed: int = 0) -> dict:
    streams_of = jax.random.split(jax.random.key(seed), 9)
    integrals = gaussian(streams_of[0], (NO, NV, NV, NV), NV ** -0.5, 0.5, ((1, 4),))
    doubles = gaussian(streams_of[1], (NO * NO, NV, NV), 0.001, 0.0059814453, ((0, 4),))
    coulomb = gaussian(streams_of[2], (NO * NO, NV, NV), 0.03, 0.1796875, ((0, 4),))
    singles = gaussian(streams_of[3], (NO, NV), 0.03, 0.18, ((1, 4),), jnp.float32)
    occ_energy = jnp.clip(jax.random.uniform(streams_of[4], (NO,), jnp.float32, -2.0, -0.5), -2.0, -0.5)
    vir_energy = jnp.clip(jax.random.uniform(streams_of[5], (NV,), jnp.float32, 0.3, 3.0), 0.3, 3.0)
    triplets = with_ends(jax.random.randint(streams_of[6], (GROUPS, TRIP, 3), 0, NO), jax.random.fold_in(streams_of[6], 1), 0, NO - 1).astype(jnp.int32)
    tile_count = draw_tile_count(jax.random.fold_in(streams_of[8], 71), 0)
    return dict(integrals=integrals, doubles=doubles, coulomb=coulomb, singles=singles, occ_energy=occ_energy, vir_energy=vir_energy, triplets=triplets, tile_count=tile_count)


def slot_energy(integrals, doubles, coulomb, singles, occ_energy, vir_energy, triplet):
    first_occ = triplet[0]
    second_occ = triplet[1]
    third_occ = triplet[2]
    slab_rows = integrals[first_occ].reshape(NV * NV, NV)
    doubles_kj = doubles[third_occ * NO + second_occ]
    doubles_jk = doubles[second_occ * NO + third_occ]
    first = jnp.dot(slab_rows, doubles_kj.T, preferred_element_type=jnp.float32).reshape(NV, NV, NV)
    second = jnp.dot(slab_rows, doubles_jk.T, preferred_element_type=jnp.float32).reshape(NV, NV, NV)
    connected = first + jnp.transpose(second, (0, 2, 1))
    coupling = coulomb[second_occ * NO + third_occ].astype(jnp.float32)
    full = connected + singles[first_occ][:, None, None] * coupling[None, :, :]
    occ_sum = occ_energy[first_occ] + occ_energy[second_occ] + occ_energy[third_occ]
    denominator = occ_sum - vir_energy[:, None, None] - vir_energy[None, :, None] - vir_energy[None, None, :]
    return jnp.sum(full * full / denominator)


def reference(integrals, doubles, coulomb, singles, occ_energy, vir_energy, triplets, tile_count):
    flat_triplets = triplets.reshape(GROUPS * TRIP, 3)

    def one_slot(triplet):
        return slot_energy(integrals, doubles, coulomb, singles, occ_energy, vir_energy, triplet)

    energies = lax.map(one_slot, flat_triplets).reshape(GROUPS, TRIP)
    slot_ids = jnp.arange(TRIP, dtype=jnp.int32)
    live = slot_ids[None, :] < tile_count[:, None]
    triplet_energy = jnp.where(live, energies, jnp.zeros_like(energies))
    mean_energy = jnp.sum(triplet_energy) / (GROUPS * TRIP)
    return triplet_energy, mean_energy
```

```python
import functools

import jax
import jax.numpy as jnp
from jax import lax
from jax.experimental import pallas as pl
from jax.experimental.pallas import tpu as pltpu
from jax.sharding import PartitionSpec as P

MESH = pl.DeviceIdType.MESH


def team_count(occupied, rows, groups):
    teams = occupied
    while teams > 1 and (occupied % teams or rows % teams or groups % (2 * teams)):
        teams -= 1
    return teams


def gather_kernel(n, groups, teams, occupied, slots, doubles_ref, coulomb_ref, integrals_ref, trip_hbm, live_ref, dp_ref, cp_ref,
                  held_ref, list_ref, count_ref, all_ref, trip_ref, small_sem, held_sem, local_sem, send_sem, recv_sem, fsend_sem, frecv_sem, csend_sem, crecv_sem):
    g = lax.axis_index("grp")
    q = lax.axis_index("blk")
    rows, width = doubles_ref.shape[0], doubles_ref.shape[1]
    runs = rows // teams
    half = width // 2
    team = g // (groups // teams)
    core = g % 2
    partner = g + 1 - 2 * core
    mine = pl.ds(pl.multiple_of(core * half, half), half)
    arrays = ((doubles_ref, dp_ref), (coulomb_ref, cp_ref))

    barrier = pltpu.get_barrier_semaphore()
    for dg in range(1, groups):
        pl.semaphore_signal(barrier, inc=1, device_id={"grp": (g + dg) % groups}, device_id_type=MESH)
    for dq in range(1, n):
        pl.semaphore_signal(barrier, inc=1, device_id={"blk": (q + dq) % n}, device_id_type=MESH)

    def own_row(m):
        j = (q * rows + teams * m) // occupied
        return teams * m + (team + occupied * teams - j) % teams

    small = pltpu.make_async_copy(trip_hbm, trip_ref, small_sem)
    small.start()
    locals_ = []
    for m in range(runs):
        for x, (src, dst) in enumerate(arrays):
            copy = pltpu.make_async_copy(src.at[own_row(m)], dst.at[q * runs + m], local_sem.at[m, x])
            copy.start()
            locals_.append(copy)
    share = held_ref.shape[1]
    held = pltpu.make_async_copy(integrals_ref.at[:, pl.ds(core * share, share)], held_ref, held_sem)
    held.start()
    small.wait()
    i, j, k = trip_ref[0], trip_ref[1], trip_ref[2]
    cube = occupied * occupied * occupied
    owner = lax.rem(j + k, jnp.full_like(j, teams))
    code = owner * cube + (i * occupied + j) * occupied + k
    live = lax.broadcasted_iota(jnp.int32, code.shape, 1) < live_ref[0]
    all_ref[g] = jnp.full((1, all_ref.shape[2]), -1, jnp.int32)
    all_ref[g, :, :slots] = jnp.where(live, code, -1)
    pl.semaphore_wait(barrier, groups - 1 + n - 1)

    code_copies = []
    for dg in range(1, groups):
        copy = pltpu.make_async_remote_copy(
            src_ref=all_ref.at[g], dst_ref=all_ref.at[g], send_sem=csend_sem.at[dg - 1], recv_sem=crecv_sem.at[dg - 1],
            device_id={"grp": (g + dg) % groups}, device_id_type=MESH)
        copy.start()
        code_copies.append(copy)
    sends = []
    for m in range(runs):
        for x, (src, dst) in enumerate(arrays):
            locals_[m * 2 + x].wait()
            for dq in range(1, n):
                copy = pltpu.make_async_remote_copy(
                    src_ref=dst.at[q * runs + m, mine], dst_ref=dst.at[q * runs + m, mine],
                    send_sem=send_sem.at[m, x, dq - 1], recv_sem=recv_sem.at[m, x, dq - 1],
                    device_id={"blk": (q + dq) % n}, device_id_type=MESH)
                copy.start()
                sends.append(copy)
    for copy in code_copies:
        copy.wait()
    table = all_ref[:, 0, :]
    ours = jnp.logical_and(table >= team * cube, table < (team + 1) * cube).astype(jnp.int32)
    inner = table - team * cube
    group_ids = lax.broadcasted_iota(jnp.int32, (groups, 1), 0)
    totals = jnp.sum(ours, axis=1, keepdims=True)
    before = jnp.zeros((groups, 1), jnp.int32)
    for other in range(groups):
        before += jnp.where(group_ids > other, totals[other:other + 1], 0)
    size = groups // teams // 2
    member = g // 2 % size
    places = lax.broadcasted_iota(jnp.int32, (groups, list_ref.shape[1]), 1) * size + member
    listed = jnp.zeros(places.shape, jnp.int32)
    for slot in range(slots):
        column = ours[:, slot:slot + 1]
        value = (group_ids * slots + slot) * cube + inner[:, slot:slot + 1]
        rank = jnp.where(column > 0, before, -1)
        listed += jnp.where(places == rank, value, 0)
        before += column
    list_ref[...] = jnp.sum(listed, axis=0, keepdims=True)
    whole = jnp.sum(totals, axis=0, keepdims=True)
    count_ref[...] = jnp.broadcast_to((whole - member + size - 1) // size, count_ref.shape)

    forwards = []
    at = 0
    for m in range(runs):
        for x, (src, dst) in enumerate(arrays):
            for dq in range(1, n):
                sends[at].wait_recv()
                at += 1
                piece = dst.at[((q + n - dq) % n) * runs + m, mine]
                copy = pltpu.make_async_remote_copy(
                    src_ref=piece, dst_ref=piece,
                    send_sem=fsend_sem.at[m, x, dq - 1], recv_sem=frecv_sem.at[m, x, dq - 1],
                    device_id={"grp": partner}, device_id_type=MESH)
                copy.start()
                forwards.append(copy)
    held.wait()
    for copy in sends:
        copy.wait_send()
    for copy in forwards:
        copy.wait()


def compute_kernel(groups, slots, teams, occupied, listed, counts, singles, occ, vir, integrals_ref, dp_ref, cp_ref,
                   row_ref, out_ref, vbc_ref, cf_ref):
    q = lax.axis_index("blk")
    core = lax.axis_index("grp") % 2
    blocks, width = integrals_ref.shape[1], integrals_ref.shape[2]
    count = counts[0, 0]
    last = listed.shape[1] - 1
    quads = blocks // 4
    per = max(1, 8 // quads)
    total_steps = per * quads
    lag, ranges = 2, 4

    across = jnp.broadcast_to(row_ref[...], (width, width))
    vbc_ref[...] = across + across.T
    cf_ref[...] = cp_ref[...].astype(jnp.float32)
    out_ref[...] = jnp.zeros_like(out_ref)
    rows = lax.broadcasted_iota(jnp.int32, out_ref.shape, 0)
    lanes = lax.broadcasted_iota(jnp.int32, out_ref.shape, 1)

    def decode(at):
        code = listed[0, jnp.minimum(at, last)]
        k = lax.rem(code, occupied)
        j = lax.rem(lax.div(code, occupied), occupied)
        i = lax.rem(lax.div(code, occupied * occupied), occupied)
        return i, j, k, lax.div(j * occupied + k, teams), lax.div(k * occupied + j, teams)

    def run(*accs):
        acc = [[accs[(x * ranges + r) * 2:(x * ranges + r) * 2 + 2] for r in range(ranges)] for x in range(2)]

        def push(at, quad, reg):
            i, _, _, _, kj = decode(at)
            for x in range(2):
                a = 4 * quad + 2 * x
                top = jnp.concatenate([dp_ref[kj], integrals_ref[i, a]], axis=1)
                low = jnp.concatenate([dp_ref[kj], integrals_ref[i, a + 1]], axis=1)
                pltpu.matmul_push_rhs(jnp.concatenate([top, low], axis=0), staging_register=reg, mxu_index=x, transpose=True)

        def multiply(at, quad, reg, r):
            i, _, _, jk, _ = decode(at)
            for h in range(2):
                for x in range(2):
                    left = jnp.concatenate([integrals_ref[i, 4 * quad + 2 * x + h], dp_ref[jk]], axis=1)
                    pltpu.matmul_acc_lhs(acc[x][r][h], left, load_staged_rhs=reg if h == 0 else None)

        def gather_up(at, quad, r, total):
            i, j, k, jk, _ = decode(at)
            occ_sum = occ[i] + occ[j] + occ[k]
            if quad == 0:
                total = jnp.zeros((8, width), jnp.float32)
            for h in range(2):
                for x in range(2):
                    a = core * blocks + 4 * quad + 2 * x + h
                    connected = pltpu.matmul_pop(acc[x][r][h])[:, h * width:(h + 1) * width]
                    full = connected + singles[i, a] * cf_ref[jk]
                    denominator = (occ_sum - vir[q * 2 * blocks + a]) - vbc_ref[...]
                    value = full * full / denominator
                    total = total + jnp.sum(value.reshape(width // 8, 8, width), axis=0)
            return total

        def settle(at, total):
            place = lax.div(listed[0, jnp.clip(at, 0, last)], occupied * occupied * occupied)
            real = jnp.logical_and(at >= 0, at < count)
            other, slot = jnp.where(real, lax.div(place, slots), -1), lax.rem(place, slots)
            here = jnp.logical_and(rows == other, lanes == slot)
            out_ref[...] += jnp.where(here, jnp.sum(total), 0.0)

        def finish(trip, step, total):
            at, quad = trip * per + step // quads, step % quads
            total = gather_up(jnp.maximum(at, 0), quad, step % ranges, total)
            if quad == quads - 1:
                settle(at, total)
            return total

        for side in acc:
            for pair in side:
                for one in pair:
                    pltpu.matmul_pop(one)
        push(0, 0, 0)

        def trip(b, total):
            for step in range(total_steps):
                multiply(b * per + step // quads, step % quads, step % 2, step % ranges)
                push(b * per + (step + 1) // quads, (step + 1) % quads, (step + 1) % 2)
                if step < lag:
                    total = finish(b - 1, total_steps + step - lag, total)
                else:
                    total = finish(b, step - lag, total)
            return total

        trips = lax.div(count + per - 1, per)
        total = lax.fori_loop(0, trips, trip, jnp.zeros((8, width), jnp.float32))
        for step in range(total_steps - lag, total_steps):
            total = finish(trips - 1, step, total)
        for x in range(2):
            pltpu.matmul_acc_lhs(acc[x][0][0], jnp.zeros((width, 2 * width), jnp.bfloat16), load_staged_rhs=0)
            pltpu.matmul_pop(acc[x][0][0])

    pl.run_scoped(run, *[pltpu.ACC(x)((width, 2 * width), jnp.float32) for x in range(2) for _ in range(2 * ranges)])


def reduce_kernel(n, groups, slots, part_ref, trip_ref, mean_ref, blk_buf, grp_buf, send_sem, recv_sem, gsend_sem, grecv_sem,
                  stage_ref):
    g = lax.axis_index("grp")
    q = lax.axis_index("blk")
    barrier = pltpu.get_barrier_semaphore()
    for dg in range(1, groups):
        pl.semaphore_signal(barrier, inc=1, device_id={"grp": (g + dg) % groups}, device_id_type=MESH)
    for dq in range(1, n):
        pl.semaphore_signal(barrier, inc=1, device_id={"blk": (q + dq) % n}, device_id_type=MESH)
    pl.semaphore_wait(barrier, groups - 1 + n - 1)
    copies = []
    for dq in range(1, n):
        copy = pltpu.make_async_remote_copy(
            src_ref=part_ref, dst_ref=blk_buf.at[q], send_sem=send_sem.at[dq - 1], recv_sem=recv_sem.at[dq - 1],
            device_id={"blk": (q + dq) % n}, device_id_type=MESH)
        copy.start()
        copies.append(copy)
    blk_buf[q] = part_ref[...]
    for copy in copies:
        copy.wait()
    stage = jnp.sum(blk_buf[...], axis=0)
    stage_ref[...] = stage
    grp_buf[g] = stage
    copies = []
    for dg in range(1, groups):
        copy = pltpu.make_async_remote_copy(
            src_ref=stage_ref, dst_ref=grp_buf.at[g], send_sem=gsend_sem.at[dg - 1], recv_sem=grecv_sem.at[dg - 1],
            device_id={"grp": (g + dg) % groups}, device_id_type=MESH)
        copy.start()
        copies.append(copy)
    for copy in copies:
        copy.wait()
    table = jnp.sum(grp_buf[...], axis=0)
    rows = lax.broadcasted_iota(jnp.int32, table.shape, 0)
    trip_ref[...] = jnp.sum(jnp.where(rows == g, table, 0.0), axis=0, keepdims=True)
    mean_ref[...] = jnp.sum(table, keepdims=True) / (groups * slots)


def body(n, groups, integrals, doubles, coulomb, singles, occ_energy, vir_energy, triplets, tile_count):
    occupied, _, width, _ = integrals.shape
    rows = doubles.shape[0]
    slots = triplets.shape[1]
    teams = team_count(occupied, rows, groups)
    runs = rows // teams
    pairs = n * runs
    f32, i32 = jnp.float32, jnp.int32
    vmem = pl.BlockSpec(memory_space=pltpu.VMEM)
    smem = pl.BlockSpec(memory_space=pltpu.SMEM)
    hbm = pl.BlockSpec(memory_space=pltpu.HBM)
    dma = pltpu.SemaphoreType.DMA

    row_bytes = pairs * width * width * doubles.dtype.itemsize
    spare = 1 << 20
    blocks = integrals.shape[1] // 2
    half = jax.ShapeDtypeStruct((occupied, blocks, width, width), integrals.dtype)
    keep = half.size * half.dtype.itemsize + 4 * row_bytes + 2 * spare
    lanes = -(-slots // 128) * 128
    length = -(-groups * slots // 128) * 128

    packed = jax.ShapeDtypeStruct((pairs, width, width), doubles.dtype)
    dp, cp, held, listed, counts = pl.pallas_call(
        functools.partial(gather_kernel, n, groups, teams, occupied, slots),
        out_shape=(packed, packed, half, jax.ShapeDtypeStruct((1, length), i32), jax.ShapeDtypeStruct((1, 128), i32)),
        in_specs=[hbm, hbm, hbm, hbm, smem],
        out_specs=(vmem, vmem, vmem, vmem, vmem),
        scratch_shapes=[
            pltpu.VMEM((groups, 1, lanes), i32), pltpu.VMEM((3, 1, slots), i32), dma, dma, dma((runs, 2)), dma((runs, 2, n - 1)), dma((runs, 2, n - 1)), dma((runs, 2, n - 1)), dma((runs, 2, n - 1)),
            dma((groups - 1,)), dma((groups - 1,)),
        ],
        compiler_params=pltpu.CompilerParams(collective_id=0, has_side_effects=True, vmem_limit_bytes=keep),
        name="gather",
    )(*(pltpu.with_memory_space_constraint(x, pltpu.HBM)
        for x in (doubles, coulomb, integrals, jnp.transpose(triplets, (2, 0, 1)))), tile_count)

    part = pl.pallas_call(
        functools.partial(compute_kernel, groups, slots, teams, occupied),
        out_shape=jax.ShapeDtypeStruct((groups, slots), f32),
        in_specs=[smem, smem, smem, smem, smem, vmem, vmem, vmem, vmem],
        out_specs=vmem,
        scratch_shapes=[pltpu.VMEM((width, width), f32), pltpu.VMEM((pairs, width, width), f32)],
        compiler_params=pltpu.CompilerParams(vmem_limit_bytes=keep),
        name="energy",
    )(listed, counts, singles, occ_energy, vir_energy, held, dp, cp, vir_energy.reshape(1, width))

    trip, mean = pl.pallas_call(
        functools.partial(reduce_kernel, n, groups, slots),
        out_shape=(jax.ShapeDtypeStruct((1, slots), f32), jax.ShapeDtypeStruct((1, 1), f32)),
        in_specs=[vmem],
        out_specs=(vmem, vmem),
        scratch_shapes=[
            pltpu.VMEM((n, groups, slots), f32), pltpu.VMEM((groups, groups, slots), f32),
            dma((n - 1,)), dma((n - 1,)), dma((groups - 1,)), dma((groups - 1,)), pltpu.VMEM((groups, slots), f32),
        ],
        compiler_params=pltpu.CompilerParams(collective_id=1, has_side_effects=True, vmem_limit_bytes=4 * spare),
        name="join",
    )(part)
    return trip, mean.reshape(())


def solution(mesh):
    in_specs = (
        P(None, "blk", None, None),
        P("blk", None, None),
        P("blk", None, None),
        P(None, "blk"),
        P(),
        P(),
        P("grp", None, None),
        P("grp"),
    )
    out_specs = (P("grp", None), P())
    step = functools.partial(body, mesh.shape["blk"], mesh.shape["grp"])
    return jax.shard_map(step, mesh=mesh, in_specs=in_specs, out_specs=out_specs, check_vma=False)
```

```python
import functools

import jax
import jax.numpy as jnp
from jax import lax
from jax.experimental import pallas as pl
from jax.experimental.pallas import tpu as pltpu
from jax.sharding import PartitionSpec as P

MESH = pl.DeviceIdType.MESH


def team_count(occupied, rows, groups):
    teams = occupied
    while teams > 1 and (occupied % teams or rows % teams or groups % (2 * teams)):
        teams -= 1
    return teams


def gather_kernel(n, groups, teams, occupied, slots, doubles_ref, coulomb_ref, integrals_ref, trip_hbm, live_ref, dp_ref, cp_ref,
                  held_ref, list_ref, count_ref, all_ref, trip_ref, small_sem, held_sem, local_sem, send_sem, recv_sem, fsend_sem, frecv_sem, csend_sem, crecv_sem):
    g = lax.axis_index("grp")
    q = lax.axis_index("blk")
    rows, width = doubles_ref.shape[0], doubles_ref.shape[1]
    runs = rows // teams
    half = width // 2
    team = g // (groups // teams)
    core = g % 2
    partner = g + 1 - 2 * core
    mine = pl.ds(pl.multiple_of(core * half, half), half)
    arrays = ((doubles_ref, dp_ref), (coulomb_ref, cp_ref))

    barrier = pltpu.get_barrier_semaphore()
    for dg in range(1, groups):
        pl.semaphore_signal(barrier, inc=1, device_id={"grp": (g + dg) % groups}, device_id_type=MESH)
    for dq in range(1, n):
        pl.semaphore_signal(barrier, inc=1, device_id={"blk": (q + dq) % n}, device_id_type=MESH)

    def own_row(m):
        j = (q * rows + teams * m) // occupied
        return teams * m + (team + occupied * teams - j) % teams

    small = pltpu.make_async_copy(trip_hbm, trip_ref, small_sem)
    small.start()
    locals_ = []
    for m in range(runs):
        for x, (src, dst) in enumerate(arrays):
            copy = pltpu.make_async_copy(src.at[own_row(m)], dst.at[q * runs + m], local_sem.at[m, x])
            copy.start()
            locals_.append(copy)
    share = held_ref.shape[1]
    held = pltpu.make_async_copy(integrals_ref.at[:, pl.ds(core * share, share)], held_ref, held_sem)
    held.start()
    small.wait()
    i, j, k = trip_ref[0], trip_ref[1], trip_ref[2]
    cube = occupied * occupied * occupied
    owner = lax.rem(j + k, jnp.full_like(j, teams))
    code = owner * cube + (i * occupied + j) * occupied + k
    live = lax.broadcasted_iota(jnp.int32, code.shape, 1) < live_ref[0]
    all_ref[g] = jnp.full((1, all_ref.shape[2]), -1, jnp.int32)
    all_ref[g, :, :slots] = jnp.where(live, code, -1)
    pl.semaphore_wait(barrier, groups - 1 + n - 1)

    code_copies = []
    for dg in range(1, groups):
        copy = pltpu.make_async_remote_copy(
            src_ref=all_ref.at[g], dst_ref=all_ref.at[g], send_sem=csend_sem.at[dg - 1], recv_sem=crecv_sem.at[dg - 1],
            device_id={"grp": (g + dg) % groups}, device_id_type=MESH)
        copy.start()
        code_copies.append(copy)
    sends = []
    for m in range(runs):
        for x, (src, dst) in enumerate(arrays):
            locals_[m * 2 + x].wait()
            for dq in range(1, n):
                copy = pltpu.make_async_remote_copy(
                    src_ref=dst.at[q * runs + m, mine], dst_ref=dst.at[q * runs + m, mine],
                    send_sem=send_sem.at[m, x, dq - 1], recv_sem=recv_sem.at[m, x, dq - 1],
                    device_id={"blk": (q + dq) % n}, device_id_type=MESH)
                copy.start()
                sends.append(copy)
    for copy in code_copies:
        copy.wait()
    table = all_ref[:, 0, :]
    ours = jnp.logical_and(table >= team * cube, table < (team + 1) * cube).astype(jnp.int32)
    inner = table - team * cube
    group_ids = lax.broadcasted_iota(jnp.int32, (groups, 1), 0)
    totals = jnp.sum(ours, axis=1, keepdims=True)
    before = jnp.zeros((groups, 1), jnp.int32)
    for other in range(groups):
        before += jnp.where(group_ids > other, totals[other:other + 1], 0)
    size = groups // teams // 2
    member = g // 2 % size
    places = lax.broadcasted_iota(jnp.int32, (groups, list_ref.shape[1]), 1) * size + member
    listed = jnp.zeros(places.shape, jnp.int32)
    for slot in range(slots):
        column = ours[:, slot:slot + 1]
        value = (group_ids * slots + slot) * cube + inner[:, slot:slot + 1]
        rank = jnp.where(column > 0, before, -1)
        listed += jnp.where(places == rank, value, 0)
        before += column
    list_ref[...] = jnp.sum(listed, axis=0, keepdims=True)
    whole = jnp.sum(totals, axis=0, keepdims=True)
    count_ref[...] = jnp.broadcast_to((whole - member + size - 1) // size, count_ref.shape)

    forwards = []
    at = 0
    for m in range(runs):
        for x, (src, dst) in enumerate(arrays):
            for dq in range(1, n):
                sends[at].wait_recv()
                at += 1
                piece = dst.at[((q + n - dq) % n) * runs + m, mine]
                copy = pltpu.make_async_remote_copy(
                    src_ref=piece, dst_ref=piece,
                    send_sem=fsend_sem.at[m, x, dq - 1], recv_sem=frecv_sem.at[m, x, dq - 1],
                    device_id={"grp": partner}, device_id_type=MESH)
                copy.start()
                forwards.append(copy)
    held.wait()
    for copy in sends:
        copy.wait_send()
    for copy in forwards:
        copy.wait()


def compute_kernel(groups, slots, teams, occupied, fixed, listed, counts, singles, occ, vir, integrals_ref, dp_ref, cp_ref,
                   row_ref, out_ref, vbc_ref, cf_ref):
    q = lax.axis_index("blk")
    core = lax.axis_index("grp") % 2
    blocks, width = integrals_ref.shape[1], integrals_ref.shape[2]
    count = jnp.maximum(counts[0, 0] - fixed, 0)
    last = listed.shape[1] - 1
    quads = blocks // 4
    per = max(1, 8 // quads)
    total_steps = per * quads
    lag, ranges = 2, 4

    across = jnp.broadcast_to(row_ref[...], (width, width))
    vbc_ref[...] = across + across.T
    cf_ref[...] = cp_ref[...].astype(jnp.float32)
    out_ref[...] = jnp.zeros_like(out_ref)
    rows = lax.broadcasted_iota(jnp.int32, out_ref.shape, 0)
    lanes = lax.broadcasted_iota(jnp.int32, out_ref.shape, 1)

    def decode(at):
        code = listed[0, jnp.minimum(at + fixed, last)]
        k = lax.rem(code, occupied)
        j = lax.rem(lax.div(code, occupied), occupied)
        i = lax.rem(lax.div(code, occupied * occupied), occupied)
        return i, j, k, lax.div(j * occupied + k, teams), lax.div(k * occupied + j, teams)

    def run(*accs):
        acc = [[accs[(x * ranges + r) * 2:(x * ranges + r) * 2 + 2] for r in range(ranges)] for x in range(2)]

        def push(at, quad, reg):
            i, _, _, _, kj = decode(at)
            for x in range(2):
                a = 4 * quad + 2 * x
                top = jnp.concatenate([dp_ref[kj], integrals_ref[i, a]], axis=1)
                low = jnp.concatenate([dp_ref[kj], integrals_ref[i, a + 1]], axis=1)
                pltpu.matmul_push_rhs(jnp.concatenate([top, low], axis=0), staging_register=reg, mxu_index=x, transpose=True)

        def multiply(at, quad, reg, r):
            i, _, _, jk, _ = decode(at)
            for h in range(2):
                for x in range(2):
                    left = jnp.concatenate([integrals_ref[i, 4 * quad + 2 * x + h], dp_ref[jk]], axis=1)
                    pltpu.matmul_acc_lhs(acc[x][r][h], left, load_staged_rhs=reg if h == 0 else None)

        def gather_up(at, quad, r, total):
            i, j, k, jk, _ = decode(at)
            occ_sum = occ[i] + occ[j] + occ[k]
            if quad == 0:
                total = jnp.zeros((8, width), jnp.float32)
            for h in range(2):
                for x in range(2):
                    a = core * blocks + 4 * quad + 2 * x + h
                    connected = pltpu.matmul_pop(acc[x][r][h])[:, h * width:(h + 1) * width]
                    full = connected + singles[i, a] * cf_ref[jk]
                    denominator = (occ_sum - vir[q * 2 * blocks + a]) - vbc_ref[...]
                    value = full * full / denominator
                    total = total + jnp.sum(value.reshape(width // 8, 8, width), axis=0)
            return total

        def settle(at, total):
            place = lax.div(listed[0, jnp.clip(at + fixed, 0, last)], occupied * occupied * occupied)
            real = jnp.logical_and(at >= 0, at < count)
            other, slot = jnp.where(real, lax.div(place, slots), -1), lax.rem(place, slots)
            here = jnp.logical_and(rows == other, lanes == slot)
            out_ref[...] += jnp.where(here, jnp.sum(total), 0.0)

        def finish(trip, step, total):
            at, quad = trip * per + step // quads, step % quads
            total = gather_up(jnp.maximum(at, 0), quad, step % ranges, total)
            if quad == quads - 1:
                settle(at, total)
            return total

        for side in acc:
            for pair in side:
                for one in pair:
                    pltpu.matmul_pop(one)
        push(0, 0, 0)

        def trip(b, total):
            for step in range(total_steps):
                multiply(b * per + step // quads, step % quads, step % 2, step % ranges)
                push(b * per + (step + 1) // quads, (step + 1) % quads, (step + 1) % 2)
                if step < lag:
                    total = finish(b - 1, total_steps + step - lag, total)
                else:
                    total = finish(b, step - lag, total)
            return total

        trips = lax.div(count + per - 1, per)
        total = lax.fori_loop(0, trips, trip, jnp.zeros((8, width), jnp.float32))
        for step in range(total_steps - lag, total_steps):
            total = finish(trips - 1, step, total)
        for x in range(2):
            pltpu.matmul_acc_lhs(acc[x][0][0], jnp.zeros((width, 2 * width), jnp.bfloat16), load_staged_rhs=0)
            pltpu.matmul_pop(acc[x][0][0])

    pl.run_scoped(run, *[pltpu.ACC(x)((width, 2 * width), jnp.float32) for x in range(2) for _ in range(2 * ranges)])


def reduce_kernel(n, groups, slots, teams, occupied, fixed, batch, listed, counts, singles, occ, vir, integrals_ref, dp_ref, cp_ref, row_ref,
                  part_ref, trip_ref, mean_ref, blk_buf, grp_buf, send_sem, recv_sem, gsend_sem, grecv_sem, stage_ref, own_ref, vbc_ref):
    g = lax.axis_index("grp")
    q = lax.axis_index("blk")
    barrier = pltpu.get_barrier_semaphore()
    for dg in range(1, groups):
        pl.semaphore_signal(barrier, inc=1, device_id={"grp": (g + dg) % groups}, device_id_type=MESH)
    for dq in range(1, n):
        pl.semaphore_signal(barrier, inc=1, device_id={"blk": (q + dq) % n}, device_id_type=MESH)

    blocks, width = integrals_ref.shape[1], integrals_ref.shape[2]
    first = (g % 2) * blocks
    across = jnp.broadcast_to(row_ref[...], (width, width))
    vbc_ref[...] = across + across.T
    count = counts[0, 0]
    spots = lax.broadcasted_iota(jnp.int32, part_ref.shape, 0) * slots + lax.broadcasted_iota(jnp.int32, part_ref.shape, 1)
    contract = (((1,), (1,)), ((), ()))

    def step(b, table):
        for u in range(batch):
            at = b * batch + u
            code = listed[0, at]
            k = lax.rem(code, occupied)
            j = lax.rem(lax.div(code, occupied), occupied)
            i = lax.rem(lax.div(code, occupied * occupied), occupied)
            place = lax.div(code, occupied * occupied * occupied)
            jk = lax.div(j * occupied + k, teams)
            kj = lax.div(k * occupied + j, teams)
            occ_sum = occ[i] + occ[j] + occ[k]
            d_jk, d_kj = dp_ref[jk], dp_ref[kj]
            total = jnp.zeros((8, width), jnp.float32)
            for a in range(blocks):
                block = integrals_ref[i, a]
                left = jnp.concatenate([block, d_jk], axis=1)
                right = jnp.concatenate([d_kj, block], axis=1)
                connected = lax.dot_general(left, right, contract, preferred_element_type=jnp.float32)
                full = connected + singles[i, first + a] * cp_ref[jk].astype(jnp.float32)
                denominator = (occ_sum - vir[q * 2 * blocks + first + a]) - vbc_ref[...]
                value = full * full / denominator
                total = total + jnp.sum(value.reshape(width // 8, 8, width), axis=0)
            here = jnp.logical_and(spots == place, at < count)
            table = table + jnp.where(here, jnp.sum(total), 0.0)
        return table

    own_ref[...] = lax.fori_loop(0, fixed // batch, step, part_ref[...])
    pl.semaphore_wait(barrier, groups - 1 + n - 1)
    copies = []
    for dq in range(1, n):
        copy = pltpu.make_async_remote_copy(
            src_ref=own_ref, dst_ref=blk_buf.at[q], send_sem=send_sem.at[dq - 1], recv_sem=recv_sem.at[dq - 1],
            device_id={"blk": (q + dq) % n}, device_id_type=MESH)
        copy.start()
        copies.append(copy)
    blk_buf[q] = own_ref[...]
    for copy in copies:
        copy.wait()
    stage = jnp.sum(blk_buf[...], axis=0)
    stage_ref[...] = stage
    grp_buf[g] = stage
    copies = []
    for dg in range(1, groups):
        copy = pltpu.make_async_remote_copy(
            src_ref=stage_ref, dst_ref=grp_buf.at[g], send_sem=gsend_sem.at[dg - 1], recv_sem=grecv_sem.at[dg - 1],
            device_id={"grp": (g + dg) % groups}, device_id_type=MESH)
        copy.start()
        copies.append(copy)
    for copy in copies:
        copy.wait()
    table = jnp.sum(grp_buf[...], axis=0)
    rows = lax.broadcasted_iota(jnp.int32, table.shape, 0)
    trip_ref[...] = jnp.sum(jnp.where(rows == g, table, 0.0), axis=0, keepdims=True)
    mean_ref[...] = jnp.sum(table, keepdims=True) / (groups * slots)


def body(n, groups, integrals, doubles, coulomb, singles, occ_energy, vir_energy, triplets, tile_count):
    occupied, _, width, _ = integrals.shape
    rows = doubles.shape[0]
    slots = triplets.shape[1]
    teams = team_count(occupied, rows, groups)
    runs = rows // teams
    pairs = n * runs
    f32, i32 = jnp.float32, jnp.int32
    vmem = pl.BlockSpec(memory_space=pltpu.VMEM)
    smem = pl.BlockSpec(memory_space=pltpu.SMEM)
    hbm = pl.BlockSpec(memory_space=pltpu.HBM)
    dma = pltpu.SemaphoreType.DMA

    row_bytes = pairs * width * width * doubles.dtype.itemsize
    spare = 1 << 20
    blocks = integrals.shape[1] // 2
    half = jax.ShapeDtypeStruct((occupied, blocks, width, width), integrals.dtype)
    keep = half.size * half.dtype.itemsize + 4 * row_bytes + 2 * spare
    lanes = -(-slots // 128) * 128
    length = -(-groups * slots // 128) * 128
    fixed, batch = 8, 4

    packed = jax.ShapeDtypeStruct((pairs, width, width), doubles.dtype)
    dp, cp, held, listed, counts = pl.pallas_call(
        functools.partial(gather_kernel, n, groups, teams, occupied, slots),
        out_shape=(packed, packed, half, jax.ShapeDtypeStruct((1, length), i32), jax.ShapeDtypeStruct((1, 128), i32)),
        in_specs=[hbm, hbm, hbm, hbm, smem],
        out_specs=(vmem, vmem, vmem, vmem, vmem),
        scratch_shapes=[
            pltpu.VMEM((groups, 1, lanes), i32), pltpu.VMEM((3, 1, slots), i32), dma, dma, dma((runs, 2)), dma((runs, 2, n - 1)), dma((runs, 2, n - 1)), dma((runs, 2, n - 1)), dma((runs, 2, n - 1)),
            dma((groups - 1,)), dma((groups - 1,)),
        ],
        compiler_params=pltpu.CompilerParams(collective_id=0, has_side_effects=True, vmem_limit_bytes=keep),
        name="gather",
    )(*(pltpu.with_memory_space_constraint(x, pltpu.HBM)
        for x in (doubles, coulomb, integrals, jnp.transpose(triplets, (2, 0, 1)))), tile_count)

    part = pl.pallas_call(
        functools.partial(compute_kernel, groups, slots, teams, occupied, fixed),
        out_shape=jax.ShapeDtypeStruct((groups, slots), f32),
        in_specs=[smem, smem, smem, smem, smem, vmem, vmem, vmem, vmem],
        out_specs=vmem,
        scratch_shapes=[pltpu.VMEM((width, width), f32), pltpu.VMEM((pairs, width, width), f32)],
        compiler_params=pltpu.CompilerParams(vmem_limit_bytes=keep),
        name="energy",
    )(listed, counts, singles, occ_energy, vir_energy, held, dp, cp, vir_energy.reshape(1, width))

    trip, mean = pl.pallas_call(
        functools.partial(reduce_kernel, n, groups, slots, teams, occupied, fixed, batch),
        out_shape=(jax.ShapeDtypeStruct((1, slots), f32), jax.ShapeDtypeStruct((1, 1), f32)),
        in_specs=[smem, smem, smem, smem, smem, vmem, vmem, vmem, vmem, vmem],
        out_specs=(vmem, vmem),
        scratch_shapes=[
            pltpu.VMEM((n, groups, slots), f32), pltpu.VMEM((groups, groups, slots), f32),
            dma((n - 1,)), dma((n - 1,)), dma((groups - 1,)), dma((groups - 1,)), pltpu.VMEM((groups, slots), f32),
            pltpu.VMEM((groups, slots), f32), pltpu.VMEM((width, width), f32),
        ],
        compiler_params=pltpu.CompilerParams(collective_id=1, has_side_effects=True, vmem_limit_bytes=keep),
        name="join",
    )(listed, counts, singles, occ_energy, vir_energy, held, dp, cp, vir_energy.reshape(1, width), part)
    return trip, mean.reshape(())


def solution(mesh):
    in_specs = (
        P(None, "blk", None, None),
        P("blk", None, None),
        P("blk", None, None),
        P(None, "blk"),
        P(),
        P(),
        P("grp", None, None),
        P("grp"),
    )
    out_specs = (P("grp", None), P())
    step = functools.partial(body, mesh.shape["blk"], mesh.shape["grp"])
    return jax.shard_map(step, mesh=mesh, in_specs=in_specs, out_specs=out_specs, check_vma=False)
```

```python
import functools

import jax
import jax.numpy as jnp
from jax import lax
from jax.experimental import pallas as pl
from jax.experimental.pallas import tpu as pltpu
from jax.sharding import PartitionSpec as P

MESH = pl.DeviceIdType.MESH


def team_count(occupied, rows, groups):
    teams = occupied
    while teams > 1 and (occupied % teams or rows % teams or groups % (2 * teams)):
        teams -= 1
    return teams


def gather_kernel(n, groups, teams, occupied, slots, doubles_ref, coulomb_ref, integrals_ref, trip_hbm, live_hbm, dp_ref, cp_ref,
                  held_ref, list_ref, count_ref, all_ref, trip_ref, live_ref, small_sem, held_sem, local_sem, send_sem, recv_sem,
                  fsend_sem, frecv_sem, csend_sem, crecv_sem, psend_sem, precv_sem):
    g = lax.axis_index("grp")
    q = lax.axis_index("blk")
    rows, width = doubles_ref.shape[0], doubles_ref.shape[1]
    runs = rows // teams
    half = width // 2
    chips = groups // 2
    team = g // (groups // teams)
    chip = g // 2
    core = g % 2
    partner = g + 1 - 2 * core
    mine = pl.ds(pl.multiple_of(core * half, half), half)
    arrays = ((doubles_ref, dp_ref), (coulomb_ref, cp_ref))
    square = n == 4
    peers = [q + 1 - 2 * (q % 2), q + 2 - 4 * (q // 2)] if square else [(q + d) % n for d in range(1, n)]
    has_lower = (chip + chips - 1) // chips
    has_upper = (2 * chips - 2 - chip) // chips

    barrier = pltpu.get_barrier_semaphore()
    pl.semaphore_signal(barrier, inc=1, device_id={"grp": partner}, device_id_type=MESH)
    for peer in peers:
        pl.semaphore_signal(barrier, inc=1, device_id={"blk": peer}, device_id_type=MESH)

    @pl.when(chip > 0)
    def _():
        pl.semaphore_signal(barrier, inc=1, device_id={"grp": g - 2}, device_id_type=MESH)

    @pl.when(chip < chips - 1)
    def _():
        pl.semaphore_signal(barrier, inc=1, device_id={"grp": g + 2}, device_id_type=MESH)

    def own_row(m):
        j = (q * rows + teams * m) // occupied
        return teams * m + (team + occupied * teams - j) % teams

    small = [pltpu.make_async_copy(trip_hbm, trip_ref, small_sem.at[0]), pltpu.make_async_copy(live_hbm, live_ref, small_sem.at[1])]
    for copy in small:
        copy.start()
    locals_ = []
    for m in range(runs):
        for x, (src, dst) in enumerate(arrays):
            copy = pltpu.make_async_copy(src.at[own_row(m)], dst.at[q * runs + m], local_sem.at[m, x])
            copy.start()
            locals_.append(copy)
    share = held_ref.shape[1]
    held = pltpu.make_async_copy(integrals_ref.at[:, pl.ds(core * share, share)], held_ref, held_sem)
    held.start()
    for copy in small:
        copy.wait()
    i, j, k = trip_ref[0], trip_ref[1], trip_ref[2]
    cube = occupied * occupied * occupied
    owner = lax.rem(j + k, jnp.full_like(j, teams))
    code = owner * cube + (i * occupied + j) * occupied + k
    live = lax.broadcasted_iota(jnp.int32, code.shape, 1) < live_ref[...]
    all_ref[g] = jnp.full((1, all_ref.shape[2]), -1, jnp.int32)
    all_ref[g, :, :slots] = jnp.where(live, code, -1)
    for copy in locals_:
        copy.wait()
    pl.semaphore_wait(barrier, 1 + len(peers) + has_lower + has_upper)

    def code_copy(row, way, t):
        to = {0: g + 2, 1: g - 2}[way]
        return pltpu.make_async_remote_copy(
            src_ref=all_ref.at[row], dst_ref=all_ref.at[row], send_sem=csend_sem.at[way, t], recv_sem=crecv_sem.at[way, t],
            device_id={"grp": to}, device_id_type=MESH)

    def side_copy(row, at):
        return pltpu.make_async_remote_copy(
            src_ref=all_ref.at[row], dst_ref=all_ref.at[row], send_sem=psend_sem.at[at], recv_sem=precv_sem.at[at],
            device_id={"grp": partner}, device_id_type=MESH)

    def inner(way):
        return chip < chips - 1 if way == 0 else chip > 0

    def comes(way, t):
        return chip > t if way == 0 else chip < chips - 1 - t

    def origin(way, t):
        return g - 2 - 2 * t if way == 0 else g + 2 + 2 * t

    for way in range(2):
        @pl.when(inner(way))
        def _(way=way):
            code_copy(g, way, 0).start()
    side_copy(g, 0).start()

    def code_step(t):
        for way in range(2):
            @pl.when(comes(way, t))
            def _(way=way):
                code_copy(origin(way, t), way, t).wait_recv()
                if t < chips - 2:
                    @pl.when(inner(way))
                    def _():
                        code_copy(origin(way, t), way, t + 1).start()
                side_copy(origin(way, t), 1 + way * (chips - 1) + t).start()

    def piece(owner_q, m, x):
        return arrays[x][1].at[owner_q * runs + m, mine]

    def row_copy(owner_q, m, x, peer, at):
        ref = piece(owner_q, m, x)
        return pltpu.make_async_remote_copy(
            src_ref=ref, dst_ref=ref, send_sem=send_sem.at[m, x, at], recv_sem=recv_sem.at[m, x, at],
            device_id={"blk": peer}, device_id_type=MESH)

    def pass_on(owner_q, m, x, at):
        ref = piece(owner_q, m, x)
        copy = pltpu.make_async_remote_copy(
            src_ref=ref, dst_ref=ref, send_sem=fsend_sem.at[m, x, at], recv_sem=frecv_sem.at[m, x, at],
            device_id={"grp": partner}, device_id_type=MESH)
        copy.start()
        forwards.append(copy)

    forwards = []
    sends = []
    parts = [(m, x) for m in range(runs) for x in range(2)]
    steps = list(range(chips - 1))
    if square:
        cut = len(parts) // 2
        orders = [parts, parts[cut:] + parts[:cut]]
        kept = [set(parts[:cut]), set(parts[cut:])]
        across = peers[0] + peers[1] - q
        for at in range(len(parts)):
            for w in range(2):
                m, x = orders[w][at]
                copy = row_copy(q, m, x, peers[w], w)
                copy.start()
                sends.append(copy)
        for at in range(len(parts)):
            for w in range(2):
                m, x = orders[w][at]
                row_copy(peers[w], m, x, peers[w], w).wait_recv()
                if (m, x) in kept[w]:
                    copy = row_copy(peers[w], m, x, peers[1 - w], 2)
                    copy.start()
                    sends.append(copy)
                pass_on(peers[w], m, x, w)
            if at % 3 == 0 and steps:
                code_step(steps.pop(0))
        for m, x in [p for pair in zip(orders[0][:cut], orders[1][:cut]) for p in pair]:
            row_copy(across, m, x, q, 2).wait_recv()
            pass_on(across, m, x, 2)
    else:
        for m, x in parts:
            for at, peer in enumerate(peers):
                copy = row_copy(q, m, x, peer, at)
                copy.start()
                sends.append(copy)
        for m, x in parts:
            for at in range(n - 1):
                row_copy((q + n - 1 - at) % n, m, x, q, at).wait_recv()
                pass_on((q + n - 1 - at) % n, m, x, at)
    for t in steps:
        code_step(t)

    side_copy(g, 0).wait()
    for way in range(2):
        for t in range(chips - 1):
            @pl.when(comes(way, t))
            def _(way=way, t=t):
                side_copy(origin(way, t), 1 + way * (chips - 1) + t).wait()
            @pl.when(jnp.logical_and(inner(way), comes(way, t - 1)))
            def _(way=way, t=t):
                code_copy(origin(way, t - 1), way, t).wait_send()

    table = all_ref[:, 0, :]
    ours = jnp.logical_and(table >= team * cube, table < (team + 1) * cube).astype(jnp.int32)
    within = table - team * cube
    group_ids = lax.broadcasted_iota(jnp.int32, (groups, 1), 0)
    totals = jnp.sum(ours, axis=1, keepdims=True)
    before = jnp.zeros((groups, 1), jnp.int32)
    for other in range(groups):
        before += jnp.where(group_ids > other, totals[other:other + 1], 0)
    size = chips // teams
    member = chip % size
    places = lax.broadcasted_iota(jnp.int32, (groups, list_ref.shape[1]), 1) * size + member
    listed = jnp.zeros(places.shape, jnp.int32)
    for slot in range(slots):
        column = ours[:, slot:slot + 1]
        value = (group_ids * slots + slot) * cube + within[:, slot:slot + 1]
        rank = jnp.where(column > 0, before, -1)
        listed += jnp.where(places == rank, value, 0)
        before += column
    list_ref[...] = jnp.sum(listed, axis=0, keepdims=True)
    whole = jnp.sum(totals, axis=0, keepdims=True)
    count_ref[...] = jnp.broadcast_to((whole - member + size - 1) // size, count_ref.shape)

    held.wait()
    for copy in sends:
        copy.wait_send()
    for copy in forwards:
        copy.wait()


def compute_kernel(groups, slots, teams, occupied, fixed, listed, counts, singles, occ, vir, integrals_ref, dp_ref, cp_ref,
                   row_ref, out_ref, vbc_ref, cf_ref):
    q = lax.axis_index("blk")
    core = lax.axis_index("grp") % 2
    blocks, width = integrals_ref.shape[1], integrals_ref.shape[2]
    count = jnp.maximum(counts[0, 0] - fixed, 0)
    last = listed.shape[1] - 1
    quads = blocks // 4
    per = max(1, 8 // quads)
    total_steps = per * quads
    lag, ranges = 2, 4

    across = jnp.broadcast_to(row_ref[...], (width, width))
    vbc_ref[...] = across + across.T
    cf_ref[...] = cp_ref[...].astype(jnp.float32)
    out_ref[...] = jnp.zeros_like(out_ref)
    spots = lax.broadcasted_iota(jnp.int32, out_ref.shape, 0) * out_ref.shape[1] + lax.broadcasted_iota(jnp.int32, out_ref.shape, 1)

    def decode(at):
        code = listed[0, jnp.minimum(at + fixed, last)]
        k = lax.rem(code, occupied)
        j = lax.rem(lax.div(code, occupied), occupied)
        i = lax.rem(lax.div(code, occupied * occupied), occupied)
        return i, j, k, lax.div(j * occupied + k, teams), lax.div(k * occupied + j, teams)

    def run(*accs):
        acc = [[accs[(x * ranges + r) * 2:(x * ranges + r) * 2 + 2] for r in range(ranges)] for x in range(2)]

        def push(at, quad, reg):
            i, _, _, _, kj = decode(at)
            for x in range(2):
                a = 4 * quad + 2 * x
                top = jnp.concatenate([dp_ref[kj], integrals_ref[i, a]], axis=1)
                low = jnp.concatenate([dp_ref[kj], integrals_ref[i, a + 1]], axis=1)
                pltpu.matmul_push_rhs(jnp.concatenate([top, low], axis=0), staging_register=reg, mxu_index=x, transpose=True)

        def multiply(at, quad, reg, r):
            i, _, _, jk, _ = decode(at)
            for h in range(2):
                for x in range(2):
                    left = jnp.concatenate([integrals_ref[i, 4 * quad + 2 * x + h], dp_ref[jk]], axis=1)
                    pltpu.matmul_acc_lhs(acc[x][r][h], left, load_staged_rhs=reg if h == 0 else None)

        def gather_up(at, quad, r, total):
            i, j, k, jk, _ = decode(at)
            occ_sum = occ[i] + occ[j] + occ[k]
            if quad == 0:
                total = jnp.zeros((8, width), jnp.float32)
            for h in range(2):
                for x in range(2):
                    a = core * blocks + 4 * quad + 2 * x + h
                    connected = pltpu.matmul_pop(acc[x][r][h])[:, h * width:(h + 1) * width]
                    full = connected + singles[i, a] * cf_ref[jk]
                    denominator = (occ_sum - vir[q * 2 * blocks + a]) - vbc_ref[...]
                    value = full * full / denominator
                    total = total + jnp.sum(value.reshape(width // 8, 8, width), axis=0)
            return total

        def settle(at, total):
            place = lax.div(listed[0, jnp.clip(at + fixed, 0, last)], occupied * occupied * occupied)
            real = jnp.logical_and(at >= 0, at < count)
            here = spots == jnp.where(real, place, -1)
            out_ref[...] += jnp.where(here, jnp.sum(total), 0.0)

        def finish(trip, step, total):
            at, quad = trip * per + step // quads, step % quads
            total = gather_up(jnp.maximum(at, 0), quad, step % ranges, total)
            if quad == quads - 1:
                settle(at, total)
            return total

        for side in acc:
            for pair in side:
                for one in pair:
                    pltpu.matmul_pop(one)
        push(0, 0, 0)

        def trip(b, total):
            for step in range(total_steps):
                multiply(b * per + step // quads, step % quads, step % 2, step % ranges)
                push(b * per + (step + 1) // quads, (step + 1) % quads, (step + 1) % 2)
                if step < lag:
                    total = finish(b - 1, total_steps + step - lag, total)
                else:
                    total = finish(b, step - lag, total)
            return total

        trips = lax.div(count + per - 1, per)
        total = lax.fori_loop(0, trips, trip, jnp.zeros((8, width), jnp.float32))
        for step in range(total_steps - lag, total_steps):
            total = finish(trips - 1, step, total)
        for x in range(2):
            pltpu.matmul_acc_lhs(acc[x][0][0], jnp.zeros((width, 2 * width), jnp.bfloat16), load_staged_rhs=0)
            pltpu.matmul_pop(acc[x][0][0])

    pl.run_scoped(run, *[pltpu.ACC(x)((width, 2 * width), jnp.float32) for x in range(2) for _ in range(2 * ranges)])


def reduce_kernel(n, groups, slots, teams, occupied, fixed, batch, listed, counts, singles, occ, vir, integrals_ref, dp_ref, cp_ref, row_ref,
                  part_ref, trip_ref, mean_ref, all_buf, send_sem, recv_sem, own_ref, vbc_ref):
    g = lax.axis_index("grp")
    q = lax.axis_index("blk")
    barrier = pltpu.get_barrier_semaphore()
    others = [(dg, dq) for dg in range(groups) for dq in range(n) if dg or dq]
    for dg, dq in others:
        pl.semaphore_signal(barrier, inc=1, device_id={"grp": (g + dg) % groups, "blk": (q + dq) % n}, device_id_type=MESH)

    blocks, width = integrals_ref.shape[1], integrals_ref.shape[2]
    first = (g % 2) * blocks
    across = jnp.broadcast_to(row_ref[...], (width, width))
    vbc_ref[...] = across + across.T
    count = counts[0, 0]
    spots = lax.broadcasted_iota(jnp.int32, part_ref.shape, 0) * part_ref.shape[1] + lax.broadcasted_iota(jnp.int32, part_ref.shape, 1)
    contract = (((1,), (1,)), ((), ()))

    def step(b, table):
        for u in range(batch):
            at = b * batch + u
            code = listed[0, at]
            k = lax.rem(code, occupied)
            j = lax.rem(lax.div(code, occupied), occupied)
            i = lax.rem(lax.div(code, occupied * occupied), occupied)
            place = lax.div(code, occupied * occupied * occupied)
            jk = lax.div(j * occupied + k, teams)
            kj = lax.div(k * occupied + j, teams)
            occ_sum = occ[i] + occ[j] + occ[k]
            d_jk, d_kj = dp_ref[jk], dp_ref[kj]
            total = jnp.zeros((8, width), jnp.float32)
            for a in range(blocks):
                block = integrals_ref[i, a]
                left = jnp.concatenate([block, d_jk], axis=1)
                right = jnp.concatenate([d_kj, block], axis=1)
                connected = lax.dot_general(left, right, contract, preferred_element_type=jnp.float32)
                full = connected + singles[i, first + a] * cp_ref[jk].astype(jnp.float32)
                denominator = (occ_sum - vir[q * 2 * blocks + first + a]) - vbc_ref[...]
                value = full * full / denominator
                total = total + jnp.sum(value.reshape(width // 8, 8, width), axis=0)
            here = jnp.logical_and(spots == place, at < count)
            table = table + jnp.where(here, jnp.sum(total), 0.0)
        return table

    own_ref[...] = lax.fori_loop(0, fixed // batch, step, part_ref[...])
    pl.semaphore_wait(barrier, len(others))
    copies = []
    for at, (dg, dq) in enumerate(others):
        copy = pltpu.make_async_remote_copy(
            src_ref=own_ref, dst_ref=all_buf.at[g * n + q], send_sem=send_sem.at[at], recv_sem=recv_sem.at[at],
            device_id={"grp": (g + dg) % groups, "blk": (q + dq) % n}, device_id_type=MESH)
        copy.start()
        copies.append(copy)
    all_buf[g * n + q] = own_ref[...]
    for copy in copies:
        copy.wait()
    table = jnp.sum(all_buf[...], axis=0)
    spread = lax.broadcasted_iota(jnp.int32, (slots, table.shape[1]), 1) - lax.broadcasted_iota(jnp.int32, (slots, table.shape[1]), 0)
    shown = jnp.zeros((slots, table.shape[1]), jnp.float32)
    for line in range(table.shape[0]):
        shown += jnp.where(spread == g * slots - line * table.shape[1], table[line:line + 1], 0.0)
    trip_ref[...] = jnp.sum(shown, axis=1)[None, :]
    mean_ref[...] = jnp.sum(table, keepdims=True) / (groups * slots)


def body(n, groups, integrals, doubles, coulomb, singles, occ_energy, vir_energy, triplets, tile_count):
    occupied, _, width, _ = integrals.shape
    rows = doubles.shape[0]
    slots = triplets.shape[1]
    teams = team_count(occupied, rows, groups)
    runs = rows // teams
    pairs = n * runs
    f32, i32 = jnp.float32, jnp.int32
    vmem = pl.BlockSpec(memory_space=pltpu.VMEM)
    smem = pl.BlockSpec(memory_space=pltpu.SMEM)
    hbm = pl.BlockSpec(memory_space=pltpu.HBM)
    dma = pltpu.SemaphoreType.DMA

    row_bytes = pairs * width * width * doubles.dtype.itemsize
    spare = 1 << 20
    blocks = integrals.shape[1] // 2
    half = jax.ShapeDtypeStruct((occupied, blocks, width, width), integrals.dtype)
    keep = half.size * half.dtype.itemsize + 4 * row_bytes + 2 * spare
    lanes = -(-slots // 128) * 128
    length = -(-groups * slots // 128) * 128
    fixed, batch = 8, 4
    sheet = (-(-groups * slots // 128), 128)

    packed = jax.ShapeDtypeStruct((pairs, width, width), doubles.dtype)
    dp, cp, held, listed, counts = pl.pallas_call(
        functools.partial(gather_kernel, n, groups, teams, occupied, slots),
        out_shape=(packed, packed, half, jax.ShapeDtypeStruct((1, length), i32), jax.ShapeDtypeStruct((1, 128), i32)),
        in_specs=[hbm] * 4 + [pl.BlockSpec(memory_space=pl.ANY)],
        out_specs=(vmem, vmem, vmem, vmem, vmem),
        scratch_shapes=[
            pltpu.VMEM((groups, 1, lanes), i32), pltpu.VMEM((3, 1, slots), i32), pltpu.VMEM((1, 1), i32), dma((2,)), dma, dma((runs, 2)),
            dma((runs, 2, n - 1)), dma((runs, 2, n - 1)), dma((runs, 2, n - 1)), dma((runs, 2, n - 1)),
            dma((2, groups // 2)), dma((2, groups // 2)), dma((groups,)), dma((groups,)),
        ],
        compiler_params=pltpu.CompilerParams(collective_id=0, has_side_effects=True, vmem_limit_bytes=keep),
        name="gather",
    )(*(pltpu.with_memory_space_constraint(x, pltpu.HBM)
        for x in (doubles, coulomb, integrals, jnp.transpose(triplets, (2, 0, 1)))), tile_count.reshape(1, 1))

    part = pl.pallas_call(
        functools.partial(compute_kernel, groups, slots, teams, occupied, fixed),
        out_shape=jax.ShapeDtypeStruct(sheet, f32),
        in_specs=[smem, smem, smem, smem, smem, vmem, vmem, vmem, vmem],
        out_specs=vmem,
        scratch_shapes=[pltpu.VMEM((width, width), f32), pltpu.VMEM((pairs, width, width), f32)],
        compiler_params=pltpu.CompilerParams(vmem_limit_bytes=keep),
        name="energy",
    )(listed, counts, singles, occ_energy, vir_energy, held, dp, cp, vir_energy.reshape(1, width))

    trip, mean = pl.pallas_call(
        functools.partial(reduce_kernel, n, groups, slots, teams, occupied, fixed, batch),
        out_shape=(jax.ShapeDtypeStruct((1, slots), f32), jax.ShapeDtypeStruct((1, 1), f32)),
        in_specs=[smem, smem, smem, smem, smem, vmem, vmem, vmem, vmem, vmem],
        out_specs=(vmem, vmem),
        scratch_shapes=[
            pltpu.VMEM((groups * n, *sheet), f32), dma((groups * n - 1,)), dma((groups * n - 1,)), pltpu.VMEM(sheet, f32), pltpu.VMEM((width, width), f32),
        ],
        compiler_params=pltpu.CompilerParams(collective_id=1, has_side_effects=True, vmem_limit_bytes=keep),
        name="join",
    )(listed, counts, singles, occ_energy, vir_energy, held, dp, cp, vir_energy.reshape(1, width), part)
    return trip, mean.reshape(())


def solution(mesh):
    in_specs = (
        P(None, "blk", None, None),
        P("blk", None, None),
        P("blk", None, None),
        P(None, "blk"),
        P(),
        P(),
        P("grp", None, None),
        P("grp"),
    )
    out_specs = (P("grp", None), P())
    step = functools.partial(body, mesh.shape["blk"], mesh.shape["grp"])
    return jax.shard_map(step, mesh=mesh, in_specs=in_specs, out_specs=out_specs, check_vma=False)
```

```python
import functools

import jax
import jax.numpy as jnp
from jax import lax
from jax.experimental import pallas as pl
from jax.experimental.pallas import tpu as pltpu
from jax.sharding import PartitionSpec as P

MESH = pl.DeviceIdType.MESH


def team_count(occupied, rows, groups):
    teams = occupied
    while teams > 1 and (occupied % teams or rows % teams or groups % (2 * teams)):
        teams -= 1
    return teams


def gather_kernel(n, groups, teams, occupied, slots, doubles_ref, coulomb_ref, integrals_ref, trip_hbm, live_hbm, dp_ref, cp_ref,
                  held_ref, list_ref, count_ref, all_ref, trip_ref, live_ref, small_sem, held_sem, local_sem, send_sem, recv_sem,
                  fsend_sem, frecv_sem, csend_sem, crecv_sem, psend_sem, precv_sem, know_sem):
    g = lax.axis_index("grp")
    q = lax.axis_index("blk")
    rows, width = doubles_ref.shape[0], doubles_ref.shape[1]
    runs = rows // teams
    half = width // 2
    chips = groups // 2
    team = g // (groups // teams)
    chip = g // 2
    core = g % 2
    partner = g + 1 - 2 * core
    mine = pl.ds(pl.multiple_of(core * half, half), half)
    arrays = ((doubles_ref, dp_ref), (coulomb_ref, cp_ref))
    square = n == 4
    peers = [q + 1 - 2 * (q % 2), q + 2 - 4 * (q // 2)] if square else [(q + d) % n for d in range(1, n)]
    has_lower = (chip + chips - 1) // chips
    has_upper = (2 * chips - 2 - chip) // chips

    barrier = pltpu.get_barrier_semaphore()
    pl.semaphore_signal(barrier, inc=1, device_id={"grp": partner}, device_id_type=MESH)
    for peer in peers:
        pl.semaphore_signal(barrier, inc=1, device_id={"blk": peer}, device_id_type=MESH)

    @pl.when(chip > 0)
    def _():
        pl.semaphore_signal(barrier, inc=1, device_id={"grp": g - 2}, device_id_type=MESH)

    @pl.when(chip < chips - 1)
    def _():
        pl.semaphore_signal(barrier, inc=1, device_id={"grp": g + 2}, device_id_type=MESH)

    def own_row(m):
        j = (q * rows + teams * m) // occupied
        return teams * m + (team + occupied * teams - j) % teams

    small = [pltpu.make_async_copy(trip_hbm, trip_ref, small_sem.at[0]), pltpu.make_async_copy(live_hbm, live_ref, small_sem.at[1])]
    for copy in small:
        copy.start()
    locals_ = []
    for m in range(runs):
        for x, (src, dst) in enumerate(arrays):
            copy = pltpu.make_async_copy(src.at[own_row(m)], dst.at[q * runs + m], local_sem.at[m, x])
            copy.start()
            locals_.append(copy)
    share = held_ref.shape[1]
    held = pltpu.make_async_copy(integrals_ref.at[:, pl.ds(core * share, share)], held_ref, held_sem)
    held.start()
    for copy in small:
        copy.wait()
    i, j, k = trip_ref[0], trip_ref[1], trip_ref[2]
    cube = occupied * occupied * occupied
    owner = lax.rem(j + k, jnp.full_like(j, teams))
    code = owner * cube + (i * occupied + j) * occupied + k
    live = lax.broadcasted_iota(jnp.int32, code.shape, 1) < live_ref[...]
    all_ref[g] = jnp.full((1, all_ref.shape[2]), -1, jnp.int32)
    all_ref[g, :, :slots] = jnp.where(live, code, -1)
    for copy in locals_:
        copy.wait()
    pl.semaphore_wait(barrier, 1 + len(peers) + has_lower + has_upper)

    def reach(way, d):
        return chip + d < chips if way == 0 else chip - d >= 0

    def code_copy(way, d, row):
        return pltpu.make_async_remote_copy(
            src_ref=all_ref.at[row], dst_ref=all_ref.at[row], send_sem=csend_sem.at[way, d - 1], recv_sem=crecv_sem.at[way, d - 1],
            device_id={"grp": g + 2 * d * (1 - 2 * way)}, device_id_type=MESH)

    def side_copy(row, at):
        return pltpu.make_async_remote_copy(
            src_ref=all_ref.at[row], dst_ref=all_ref.at[row], send_sem=psend_sem.at[at], recv_sem=precv_sem.at[at],
            device_id={"grp": partner}, device_id_type=MESH)

    def code_step(d):
        for way in range(2):
            @pl.when(reach(way, d))
            def _(way=way):
                if d > 1:
                    pl.semaphore_wait(know_sem.at[way, d - 1], 1)
                code_copy(way, d, g).start()
                if d + 1 < chips:
                    @pl.when(reach(1 - way, 1))
                    def _():
                        pl.semaphore_signal(know_sem.at[way, d], inc=1, device_id={"grp": g - 2 * (1 - 2 * way)}, device_id_type=MESH)

    def codes_in():
        for d in range(1, chips):
            for way in range(2):
                @pl.when(reach(1 - way, d))
                def _(way=way, d=d):
                    code_copy(way, d, g - 2 * d * (1 - 2 * way)).wait_recv()
                    side_copy(g - 2 * d * (1 - 2 * way), way * (chips - 1) + d).start()

    def piece(owner_q, m, x):
        return arrays[x][1].at[owner_q * runs + m, mine]

    def row_copy(owner_q, m, x, peer, at):
        ref = piece(owner_q, m, x)
        return pltpu.make_async_remote_copy(
            src_ref=ref, dst_ref=ref, send_sem=send_sem.at[m, x, at], recv_sem=recv_sem.at[m, x, at],
            device_id={"blk": peer}, device_id_type=MESH)

    def pass_on(owner_q, m, x, at):
        ref = piece(owner_q, m, x)
        copy = pltpu.make_async_remote_copy(
            src_ref=ref, dst_ref=ref, send_sem=fsend_sem.at[m, x, at], recv_sem=frecv_sem.at[m, x, at],
            device_id={"grp": partner}, device_id_type=MESH)
        copy.start()
        forwards.append(copy)

    forwards = []
    sends = []
    parts = [(m, x) for m in range(runs) for x in range(2)]
    steps = list(range(1, chips))
    if square:
        cut = len(parts) // 2
        orders = [parts, parts[cut:] + parts[:cut]]
        kept = [set(parts[:cut]), set(parts[cut:])]
        across = peers[0] + peers[1] - q
        for at in range(len(parts)):
            for w in range(2):
                m, x = orders[w][at]
                copy = row_copy(q, m, x, peers[w], w)
                copy.start()
                sends.append(copy)
        for d in steps[:2]:
            code_step(d)
        side_copy(g, 0).start()
        steps = steps[2:]
        for at in range(len(parts)):
            for w in range(2):
                m, x = orders[w][at]
                row_copy(peers[w], m, x, peers[w], w).wait_recv()
                if (m, x) in kept[w]:
                    copy = row_copy(peers[w], m, x, peers[1 - w], 2)
                    copy.start()
                    sends.append(copy)
                pass_on(peers[w], m, x, w)
            if steps:
                code_step(steps.pop(0))
        for d in steps:
            code_step(d)
        steps = []
        codes_in()
        for m, x in [p for pair in zip(orders[0][:cut], orders[1][:cut]) for p in pair]:
            row_copy(across, m, x, q, 2).wait_recv()
            pass_on(across, m, x, 2)
    else:
        for m, x in parts:
            for at, peer in enumerate(peers):
                copy = row_copy(q, m, x, peer, at)
                copy.start()
                sends.append(copy)
        side_copy(g, 0).start()
        for m, x in parts:
            for at in range(n - 1):
                row_copy((q + n - 1 - at) % n, m, x, q, at).wait_recv()
                pass_on((q + n - 1 - at) % n, m, x, at)
    for d in steps:
        code_step(d)
    if not square:
        codes_in()

    side_copy(g, 0).wait()
    for way in range(2):
        for d in range(1, chips):
            @pl.when(reach(1 - way, d))
            def _(way=way, d=d):
                side_copy(g - 2 * d * (1 - 2 * way), way * (chips - 1) + d).wait()
            @pl.when(reach(way, d))
            def _(way=way, d=d):
                code_copy(way, d, g).wait_send()

    table = all_ref[:, 0, :]
    ours = jnp.logical_and(table >= team * cube, table < (team + 1) * cube).astype(jnp.int32)
    within = table - team * cube
    group_ids = lax.broadcasted_iota(jnp.int32, (groups, 1), 0)
    totals = jnp.sum(ours, axis=1, keepdims=True)
    before = jnp.zeros((groups, 1), jnp.int32)
    for other in range(groups):
        before += jnp.where(group_ids > other, totals[other:other + 1], 0)
    size = chips // teams
    member = chip % size
    places = lax.broadcasted_iota(jnp.int32, (groups, list_ref.shape[1]), 1) * size + member
    listed = jnp.zeros(places.shape, jnp.int32)
    for slot in range(slots):
        column = ours[:, slot:slot + 1]
        value = (group_ids * slots + slot) * cube + within[:, slot:slot + 1]
        rank = jnp.where(column > 0, before, -1)
        listed += jnp.where(places == rank, value, 0)
        before += column
    list_ref[...] = jnp.sum(listed, axis=0, keepdims=True)
    whole = jnp.sum(totals, axis=0, keepdims=True)
    count_ref[...] = jnp.broadcast_to((whole - member + size - 1) // size, count_ref.shape)

    held.wait()
    for copy in sends:
        copy.wait_send()
    for copy in forwards:
        copy.wait()


def compute_kernel(groups, slots, teams, occupied, fixed, listed, counts, singles, occ, vir, integrals_ref, dp_ref, cp_ref,
                   row_ref, out_ref, vbc_ref, cf_ref):
    q = lax.axis_index("blk")
    core = lax.axis_index("grp") % 2
    blocks, width = integrals_ref.shape[1], integrals_ref.shape[2]
    count = jnp.maximum(counts[0, 0] - fixed, 0)
    last = listed.shape[1] - 1
    quads = blocks // 4
    per = max(1, 8 // quads)
    total_steps = per * quads
    lag, ranges = 2, 4

    across = jnp.broadcast_to(row_ref[...], (width, width))
    vbc_ref[...] = across + across.T
    cf_ref[...] = cp_ref[...].astype(jnp.float32)
    out_ref[...] = jnp.zeros_like(out_ref)
    spots = lax.broadcasted_iota(jnp.int32, out_ref.shape, 0) * out_ref.shape[1] + lax.broadcasted_iota(jnp.int32, out_ref.shape, 1)

    def decode(at):
        code = listed[0, jnp.minimum(at + fixed, last)]
        k = lax.rem(code, occupied)
        j = lax.rem(lax.div(code, occupied), occupied)
        i = lax.rem(lax.div(code, occupied * occupied), occupied)
        return i, j, k, lax.div(j * occupied + k, teams), lax.div(k * occupied + j, teams)

    def run(*accs):
        acc = [[accs[(x * ranges + r) * 2:(x * ranges + r) * 2 + 2] for r in range(ranges)] for x in range(2)]

        def push(at, quad, reg):
            i, _, _, _, kj = decode(at)
            for x in range(2):
                a = 4 * quad + 2 * x
                top = jnp.concatenate([dp_ref[kj], integrals_ref[i, a]], axis=1)
                low = jnp.concatenate([dp_ref[kj], integrals_ref[i, a + 1]], axis=1)
                pltpu.matmul_push_rhs(jnp.concatenate([top, low], axis=0), staging_register=reg, mxu_index=x, transpose=True)

        def multiply(at, quad, reg, r):
            i, _, _, jk, _ = decode(at)
            for h in range(2):
                for x in range(2):
                    left = jnp.concatenate([integrals_ref[i, 4 * quad + 2 * x + h], dp_ref[jk]], axis=1)
                    pltpu.matmul_acc_lhs(acc[x][r][h], left, load_staged_rhs=reg if h == 0 else None)

        def gather_up(at, quad, r, total):
            i, j, k, jk, _ = decode(at)
            occ_sum = occ[i] + occ[j] + occ[k]
            if quad == 0:
                total = jnp.zeros((8, width), jnp.float32)
            for h in range(2):
                for x in range(2):
                    a = core * blocks + 4 * quad + 2 * x + h
                    connected = pltpu.matmul_pop(acc[x][r][h])[:, h * width:(h + 1) * width]
                    full = connected + singles[i, a] * cf_ref[jk]
                    denominator = (occ_sum - vir[q * 2 * blocks + a]) - vbc_ref[...]
                    value = full * full / denominator
                    total = total + jnp.sum(value.reshape(width // 8, 8, width), axis=0)
            return total

        def settle(at, total):
            place = lax.div(listed[0, jnp.clip(at + fixed, 0, last)], occupied * occupied * occupied)
            real = jnp.logical_and(at >= 0, at < count)
            here = spots == jnp.where(real, place, -1)
            out_ref[...] += jnp.where(here, jnp.sum(total), 0.0)

        def finish(trip, step, total):
            at, quad = trip * per + step // quads, step % quads
            total = gather_up(jnp.maximum(at, 0), quad, step % ranges, total)
            if quad == quads - 1:
                settle(at, total)
            return total

        for side in acc:
            for pair in side:
                for one in pair:
                    pltpu.matmul_pop(one)
        push(0, 0, 0)

        def trip(b, total):
            for step in range(total_steps):
                multiply(b * per + step // quads, step % quads, step % 2, step % ranges)
                push(b * per + (step + 1) // quads, (step + 1) % quads, (step + 1) % 2)
                if step < lag:
                    total = finish(b - 1, total_steps + step - lag, total)
                else:
                    total = finish(b, step - lag, total)
            return total

        trips = lax.div(count + per - 1, per)
        total = lax.fori_loop(0, trips, trip, jnp.zeros((8, width), jnp.float32))
        for step in range(total_steps - lag, total_steps):
            total = finish(trips - 1, step, total)
        for x in range(2):
            pltpu.matmul_acc_lhs(acc[x][0][0], jnp.zeros((width, 2 * width), jnp.bfloat16), load_staged_rhs=0)
            pltpu.matmul_pop(acc[x][0][0])

    pl.run_scoped(run, *[pltpu.ACC(x)((width, 2 * width), jnp.float32) for x in range(2) for _ in range(2 * ranges)])


def reduce_kernel(n, groups, slots, teams, occupied, fixed, batch, listed, counts, singles, occ, vir, integrals_ref, dp_ref, cp_ref, row_ref,
                  part_ref, trip_ref, mean_ref, all_buf, send_sem, recv_sem, own_ref, vbc_ref):
    g = lax.axis_index("grp")
    q = lax.axis_index("blk")
    barrier = pltpu.get_barrier_semaphore()
    others = [(dg, dq) for dg in range(groups) for dq in range(n) if dg or dq]
    for dg, dq in others:
        pl.semaphore_signal(barrier, inc=1, device_id={"grp": (g + dg) % groups, "blk": (q + dq) % n}, device_id_type=MESH)

    blocks, width = integrals_ref.shape[1], integrals_ref.shape[2]
    first = (g % 2) * blocks
    across = jnp.broadcast_to(row_ref[...], (width, width))
    vbc_ref[...] = across + across.T
    count = counts[0, 0]
    spots = lax.broadcasted_iota(jnp.int32, part_ref.shape, 0) * part_ref.shape[1] + lax.broadcasted_iota(jnp.int32, part_ref.shape, 1)
    contract = (((1,), (1,)), ((), ()))

    def step(b, table):
        for u in range(batch):
            at = b * batch + u
            code = listed[0, at]
            k = lax.rem(code, occupied)
            j = lax.rem(lax.div(code, occupied), occupied)
            i = lax.rem(lax.div(code, occupied * occupied), occupied)
            place = lax.div(code, occupied * occupied * occupied)
            jk = lax.div(j * occupied + k, teams)
            kj = lax.div(k * occupied + j, teams)
            occ_sum = occ[i] + occ[j] + occ[k]
            d_jk, d_kj = dp_ref[jk], dp_ref[kj]
            total = jnp.zeros((8, width), jnp.float32)
            for a in range(blocks):
                block = integrals_ref[i, a]
                left = jnp.concatenate([block, d_jk], axis=1)
                right = jnp.concatenate([d_kj, block], axis=1)
                connected = lax.dot_general(left, right, contract, preferred_element_type=jnp.float32)
                full = connected + singles[i, first + a] * cp_ref[jk].astype(jnp.float32)
                denominator = (occ_sum - vir[q * 2 * blocks + first + a]) - vbc_ref[...]
                value = full * full / denominator
                total = total + jnp.sum(value.reshape(width // 8, 8, width), axis=0)
            here = jnp.logical_and(spots == place, at < count)
            table = table + jnp.where(here, jnp.sum(total), 0.0)
        return table

    own_ref[...] = lax.fori_loop(0, fixed // batch, step, part_ref[...])
    pl.semaphore_wait(barrier, len(others))
    copies = []
    for at, (dg, dq) in enumerate(others):
        copy = pltpu.make_async_remote_copy(
            src_ref=own_ref, dst_ref=all_buf.at[g * n + q], send_sem=send_sem.at[at], recv_sem=recv_sem.at[at],
            device_id={"grp": (g + dg) % groups, "blk": (q + dq) % n}, device_id_type=MESH)
        copy.start()
        copies.append(copy)
    all_buf[g * n + q] = own_ref[...]
    for copy in copies:
        copy.wait()
    table = jnp.sum(all_buf[...], axis=0)
    spread = lax.broadcasted_iota(jnp.int32, (slots, table.shape[1]), 1) - lax.broadcasted_iota(jnp.int32, (slots, table.shape[1]), 0)
    shown = jnp.zeros((slots, table.shape[1]), jnp.float32)
    for line in range(table.shape[0]):
        shown += jnp.where(spread == g * slots - line * table.shape[1], table[line:line + 1], 0.0)
    trip_ref[...] = jnp.sum(shown, axis=1)[None, :]
    mean_ref[...] = jnp.sum(table, keepdims=True) / (groups * slots)


def body(n, groups, integrals, doubles, coulomb, singles, occ_energy, vir_energy, triplets, tile_count):
    occupied, _, width, _ = integrals.shape
    rows = doubles.shape[0]
    slots = triplets.shape[1]
    teams = team_count(occupied, rows, groups)
    runs = rows // teams
    pairs = n * runs
    f32, i32 = jnp.float32, jnp.int32
    vmem = pl.BlockSpec(memory_space=pltpu.VMEM)
    smem = pl.BlockSpec(memory_space=pltpu.SMEM)
    hbm = pl.BlockSpec(memory_space=pltpu.HBM)
    dma = pltpu.SemaphoreType.DMA

    row_bytes = pairs * width * width * doubles.dtype.itemsize
    spare = 1 << 20
    blocks = integrals.shape[1] // 2
    half = jax.ShapeDtypeStruct((occupied, blocks, width, width), integrals.dtype)
    keep = half.size * half.dtype.itemsize + 4 * row_bytes + 2 * spare
    lanes = -(-slots // 128) * 128
    length = -(-groups * slots // 128) * 128
    fixed, batch = 8, 4
    sheet = (-(-groups * slots // 128), 128)

    packed = jax.ShapeDtypeStruct((pairs, width, width), doubles.dtype)
    dp, cp, held, listed, counts = pl.pallas_call(
        functools.partial(gather_kernel, n, groups, teams, occupied, slots),
        out_shape=(packed, packed, half, jax.ShapeDtypeStruct((1, length), i32), jax.ShapeDtypeStruct((1, 128), i32)),
        in_specs=[hbm] * 4 + [pl.BlockSpec(memory_space=pl.ANY)],
        out_specs=(vmem, vmem, vmem, vmem, vmem),
        scratch_shapes=[
            pltpu.VMEM((groups, 1, lanes), i32), pltpu.VMEM((3, 1, slots), i32), pltpu.VMEM((1, 1), i32), dma((2,)), dma, dma((runs, 2)),
            dma((runs, 2, n - 1)), dma((runs, 2, n - 1)), dma((runs, 2, n - 1)), dma((runs, 2, n - 1)),
            dma((2, groups // 2)), dma((2, groups // 2)), dma((groups,)), dma((groups,)), pltpu.SemaphoreType.REGULAR((2, groups // 2)),
        ],
        compiler_params=pltpu.CompilerParams(collective_id=0, has_side_effects=True, vmem_limit_bytes=keep),
        name="gather",
    )(*(pltpu.with_memory_space_constraint(x, pltpu.HBM)
        for x in (doubles, coulomb, integrals, jnp.transpose(triplets, (2, 0, 1)))), tile_count.reshape(1, 1))

    part = pl.pallas_call(
        functools.partial(compute_kernel, groups, slots, teams, occupied, fixed),
        out_shape=jax.ShapeDtypeStruct(sheet, f32),
        in_specs=[smem, smem, smem, smem, smem, vmem, vmem, vmem, vmem],
        out_specs=vmem,
        scratch_shapes=[pltpu.VMEM((width, width), f32), pltpu.VMEM((pairs, width, width), f32)],
        compiler_params=pltpu.CompilerParams(vmem_limit_bytes=keep),
        name="energy",
    )(listed, counts, singles, occ_energy, vir_energy, held, dp, cp, vir_energy.reshape(1, width))

    trip, mean = pl.pallas_call(
        functools.partial(reduce_kernel, n, groups, slots, teams, occupied, fixed, batch),
        out_shape=(jax.ShapeDtypeStruct((1, slots), f32), jax.ShapeDtypeStruct((1, 1), f32)),
        in_specs=[smem, smem, smem, smem, smem, vmem, vmem, vmem, vmem, vmem],
        out_specs=(vmem, vmem),
        scratch_shapes=[
            pltpu.VMEM((groups * n, *sheet), f32), dma((groups * n - 1,)), dma((groups * n - 1,)), pltpu.VMEM(sheet, f32), pltpu.VMEM((width, width), f32),
        ],
        compiler_params=pltpu.CompilerParams(collective_id=1, has_side_effects=True, vmem_limit_bytes=keep),
        name="join",
    )(listed, counts, singles, occ_energy, vir_energy, held, dp, cp, vir_energy.reshape(1, width), part)
    return trip, mean.reshape(())


def solution(mesh):
    in_specs = (
        P(None, "blk", None, None),
        P("blk", None, None),
        P("blk", None, None),
        P(None, "blk"),
        P(),
        P(),
        P("grp", None, None),
        P("grp"),
    )
    out_specs = (P("grp", None), P())
    step = functools.partial(body, mesh.shape["blk"], mesh.shape["grp"])
    return jax.shard_map(step, mesh=mesh, in_specs=in_specs, out_specs=out_specs, check_vma=False)
```

```python
import functools

import jax
import jax.numpy as jnp
from jax import lax
from jax.experimental import pallas as pl
from jax.experimental.pallas import tpu as pltpu
from jax.sharding import PartitionSpec as P

MESH = pl.DeviceIdType.MESH


def team_count(occupied, rows, groups):
    teams = occupied
    while teams > 1 and (occupied % teams or rows % teams or groups % (2 * teams)):
        teams -= 1
    return teams


def gather_kernel(n, groups, teams, occupied, slots, doubles_ref, coulomb_ref, integrals_ref, trip_hbm, live_hbm, dp_ref, cp_ref,
                  held_ref, list_ref, count_ref, all_ref, trip_ref, live_ref, small_sem, held_sem, local_sem, send_sem, recv_sem,
                  fsend_sem, frecv_sem, csend_sem, crecv_sem, psend_sem, precv_sem, know_sem):
    g = lax.axis_index("grp")
    q = lax.axis_index("blk")
    rows, width = doubles_ref.shape[0], doubles_ref.shape[1]
    runs = rows // teams
    half = width // 2
    chips = groups // 2
    team = g // (groups // teams)
    chip = g // 2
    core = g % 2
    partner = g + 1 - 2 * core
    mine = pl.ds(pl.multiple_of(core * half, half), half)
    arrays = ((doubles_ref, dp_ref), (coulomb_ref, cp_ref))
    square = n == 4
    peers = [q + 1 - 2 * (q % 2), q + 2 - 4 * (q // 2)] if square else [(q + d) % n for d in range(1, n)]
    has_lower = (chip + chips - 1) // chips
    has_upper = (2 * chips - 2 - chip) // chips

    barrier = pltpu.get_barrier_semaphore()
    pl.semaphore_signal(barrier, inc=1, device_id={"grp": partner}, device_id_type=MESH)
    for peer in peers:
        pl.semaphore_signal(barrier, inc=1, device_id={"blk": peer}, device_id_type=MESH)

    @pl.when(chip > 0)
    def _():
        pl.semaphore_signal(barrier, inc=1, device_id={"grp": g - 2}, device_id_type=MESH)

    @pl.when(chip < chips - 1)
    def _():
        pl.semaphore_signal(barrier, inc=1, device_id={"grp": g + 2}, device_id_type=MESH)

    def own_row(m):
        j = (q * rows + teams * m) // occupied
        return teams * m + (team + occupied * teams - j) % teams

    small = [pltpu.make_async_copy(trip_hbm, trip_ref, small_sem.at[0]), pltpu.make_async_copy(live_hbm, live_ref, small_sem.at[1])]
    for copy in small:
        copy.start()
    locals_ = []
    for m in range(runs):
        for x, (src, dst) in enumerate(arrays):
            copy = pltpu.make_async_copy(src.at[own_row(m)], dst.at[q * runs + m], local_sem.at[m, x])
            copy.start()
            locals_.append(copy)
    share = held_ref.shape[1]
    held = pltpu.make_async_copy(integrals_ref.at[:, pl.ds(core * share, share)], held_ref, held_sem)
    held.start()
    for copy in small:
        copy.wait()
    i, j, k = trip_ref[0], trip_ref[1], trip_ref[2]
    cube = occupied * occupied * occupied
    owner = lax.rem(j + k, jnp.full_like(j, teams))
    code = owner * cube + (i * occupied + j) * occupied + k
    live = lax.broadcasted_iota(jnp.int32, code.shape, 1) < live_ref[...]
    all_ref[g] = jnp.full((1, all_ref.shape[2]), -1, jnp.int32)
    all_ref[g, :, :slots] = jnp.where(live, code, -1)
    for copy in locals_:
        copy.wait()
    pl.semaphore_wait(barrier, 1 + len(peers) + has_lower + has_upper)

    def reach(way, d):
        return chip + d < chips if way == 0 else chip - d >= 0

    def code_copy(way, d, row):
        return pltpu.make_async_remote_copy(
            src_ref=all_ref.at[row], dst_ref=all_ref.at[row], send_sem=csend_sem.at[way, d - 1], recv_sem=crecv_sem.at[way, d - 1],
            device_id={"grp": g + 2 * d * (1 - 2 * way)}, device_id_type=MESH)

    def side_copy(row, at):
        return pltpu.make_async_remote_copy(
            src_ref=all_ref.at[row], dst_ref=all_ref.at[row], send_sem=psend_sem.at[at], recv_sem=precv_sem.at[at],
            device_id={"grp": partner}, device_id_type=MESH)

    def code_step(d):
        for way in range(2):
            @pl.when(reach(way, d))
            def _(way=way):
                if d > 1:
                    pl.semaphore_wait(know_sem.at[way, d - 1], 1)
                code_copy(way, d, g).start()
                if d + 1 < chips:
                    @pl.when(reach(1 - way, 1))
                    def _():
                        pl.semaphore_signal(know_sem.at[way, d], inc=1, device_id={"grp": g - 2 * (1 - 2 * way)}, device_id_type=MESH)

    def codes_in():
        for d in range(1, chips):
            for way in range(2):
                @pl.when(reach(1 - way, d))
                def _(way=way, d=d):
                    code_copy(way, d, g - 2 * d * (1 - 2 * way)).wait_recv()
                    side_copy(g - 2 * d * (1 - 2 * way), way * (chips - 1) + d).start()

    def piece(owner_q, m, x):
        return arrays[x][1].at[owner_q * runs + m, mine]

    def row_copy(owner_q, m, x, peer, at):
        ref = piece(owner_q, m, x)
        return pltpu.make_async_remote_copy(
            src_ref=ref, dst_ref=ref, send_sem=send_sem.at[m, x, at], recv_sem=recv_sem.at[m, x, at],
            device_id={"blk": peer}, device_id_type=MESH)

    def pass_on(owner_q, m, x, at):
        ref = piece(owner_q, m, x)
        copy = pltpu.make_async_remote_copy(
            src_ref=ref, dst_ref=ref, send_sem=fsend_sem.at[m, x, at], recv_sem=frecv_sem.at[m, x, at],
            device_id={"grp": partner}, device_id_type=MESH)
        copy.start()
        forwards.append(copy)

    forwards = []
    sends = []
    parts = [(m, x) for m in range(runs) for x in range(2)]
    steps = list(range(1, chips))
    if square:
        cut = len(parts) // 2
        orders = [parts, parts[cut:] + parts[:cut]]
        kept = [set(parts[:cut]), set(parts[cut:])]
        across = peers[0] + peers[1] - q
        for at in range(len(parts)):
            for w in range(2):
                m, x = orders[w][at]
                copy = row_copy(q, m, x, peers[w], w)
                copy.start()
                sends.append(copy)
        for d in steps[:2]:
            code_step(d)
        side_copy(g, 0).start()
        steps = steps[2:]
        for at in range(len(parts)):
            for w in range(2):
                m, x = orders[w][at]
                row_copy(peers[w], m, x, peers[w], w).wait_recv()
                if (m, x) in kept[w]:
                    copy = row_copy(peers[w], m, x, peers[1 - w], 2)
                    copy.start()
                    sends.append(copy)
                pass_on(peers[w], m, x, w)
            if steps:
                code_step(steps.pop(0))
        for d in steps:
            code_step(d)
        steps = []
        codes_in()
        for m, x in [p for pair in zip(orders[0][:cut], orders[1][:cut]) for p in pair]:
            row_copy(across, m, x, q, 2).wait_recv()
            pass_on(across, m, x, 2)
    else:
        for m, x in parts:
            for at, peer in enumerate(peers):
                copy = row_copy(q, m, x, peer, at)
                copy.start()
                sends.append(copy)
        side_copy(g, 0).start()
        for m, x in parts:
            for at in range(n - 1):
                row_copy((q + n - 1 - at) % n, m, x, q, at).wait_recv()
                pass_on((q + n - 1 - at) % n, m, x, at)
    for d in steps:
        code_step(d)
    if not square:
        codes_in()

    side_copy(g, 0).wait()
    for way in range(2):
        for d in range(1, chips):
            @pl.when(reach(1 - way, d))
            def _(way=way, d=d):
                side_copy(g - 2 * d * (1 - 2 * way), way * (chips - 1) + d).wait()
            @pl.when(reach(way, d))
            def _(way=way, d=d):
                code_copy(way, d, g).wait_send()

    table = all_ref[:, 0, :]
    ours = jnp.logical_and(table >= team * cube, table < (team + 1) * cube).astype(jnp.int32)
    within = table - team * cube
    group_ids = lax.broadcasted_iota(jnp.int32, (groups, 1), 0)
    totals = jnp.sum(ours, axis=1, keepdims=True)
    before = jnp.zeros((groups, 1), jnp.int32)
    for other in range(groups):
        before += jnp.where(group_ids > other, totals[other:other + 1], 0)
    size = chips // teams
    member = chip % size
    places = lax.broadcasted_iota(jnp.int32, (groups, list_ref.shape[1]), 1) * size + member
    listed = jnp.zeros(places.shape, jnp.int32)
    for slot in range(slots):
        column = ours[:, slot:slot + 1]
        value = (group_ids * slots + slot) * cube + within[:, slot:slot + 1]
        rank = jnp.where(column > 0, before, -1)
        listed += jnp.where(places == rank, value, 0)
        before += column
    list_ref[...] = jnp.sum(listed, axis=0, keepdims=True)
    whole = jnp.sum(totals, axis=0, keepdims=True)
    count_ref[...] = jnp.broadcast_to((whole - member + size - 1) // size, count_ref.shape)

    held.wait()
    for copy in sends:
        copy.wait_send()
    for copy in forwards:
        copy.wait()


def compute_kernel(groups, slots, teams, occupied, fixed, listed, counts, singles, occ, vir, integrals_ref, dp_ref, cp_ref,
                   row_ref, out_ref, vbc_ref, cf_ref):
    q = lax.axis_index("blk")
    core = lax.axis_index("grp") % 2
    blocks, width = integrals_ref.shape[1], integrals_ref.shape[2]
    count = jnp.maximum(counts[0, 0] - fixed, 0)
    last = listed.shape[1] - 1
    quads = blocks // 4
    per = max(1, 8 // quads)
    total_steps = per * quads
    lag, ranges = 2, 4

    across = jnp.broadcast_to(row_ref[...], (width, width))
    vbc_ref[...] = across + across.T
    cf_ref[...] = cp_ref[...].astype(jnp.float32)
    out_ref[...] = jnp.zeros_like(out_ref)
    spots = lax.broadcasted_iota(jnp.int32, out_ref.shape, 0) * out_ref.shape[1] + lax.broadcasted_iota(jnp.int32, out_ref.shape, 1)

    def decode(at):
        code = listed[0, jnp.minimum(at + fixed, last)]
        k = lax.rem(code, occupied)
        j = lax.rem(lax.div(code, occupied), occupied)
        i = lax.rem(lax.div(code, occupied * occupied), occupied)
        return i, j, k, lax.div(j * occupied + k, teams), lax.div(k * occupied + j, teams)

    def run(*accs):
        acc = [[accs[(x * ranges + r) * 2:(x * ranges + r) * 2 + 2] for r in range(ranges)] for x in range(2)]

        def push(at, quad, reg):
            i, _, _, _, kj = decode(at)
            for x in range(2):
                a = 4 * quad + 2 * x
                top = jnp.concatenate([dp_ref[kj], integrals_ref[i, a]], axis=1)
                low = jnp.concatenate([dp_ref[kj], integrals_ref[i, a + 1]], axis=1)
                pltpu.matmul_push_rhs(jnp.concatenate([top, low], axis=0), staging_register=reg, mxu_index=x, transpose=True)

        def multiply(at, quad, reg, r):
            i, _, _, jk, _ = decode(at)
            for h in range(2):
                for x in range(2):
                    left = jnp.concatenate([integrals_ref[i, 4 * quad + 2 * x + h], dp_ref[jk]], axis=1)
                    pltpu.matmul_acc_lhs(acc[x][r][h], left, load_staged_rhs=reg if h == 0 else None)

        def gather_up(at, quad, r, total):
            i, j, k, jk, _ = decode(at)
            occ_sum = occ[i] + occ[j] + occ[k]
            if quad == 0:
                total = jnp.zeros((8, width), jnp.float32)
            for h in range(2):
                for x in range(2):
                    a = core * blocks + 4 * quad + 2 * x + h
                    connected = pltpu.matmul_pop(acc[x][r][h])[:, h * width:(h + 1) * width]
                    full = connected + singles[i, a] * cf_ref[jk]
                    denominator = (occ_sum - vir[q * 2 * blocks + a]) - vbc_ref[...]
                    value = full * full / denominator
                    total = total + jnp.sum(value.reshape(width // 8, 8, width), axis=0)
            return total

        def settle(at, total):
            place = lax.div(listed[0, jnp.clip(at + fixed, 0, last)], occupied * occupied * occupied)
            real = jnp.logical_and(at >= 0, at < count)
            here = spots == jnp.where(real, place, -1)
            out_ref[...] += jnp.where(here, jnp.sum(total), 0.0)

        def finish(trip, step, total):
            at, quad = trip * per + step // quads, step % quads
            total = gather_up(jnp.maximum(at, 0), quad, step % ranges, total)
            if quad == quads - 1:
                settle(at, total)
            return total

        for side in acc:
            for pair in side:
                for one in pair:
                    pltpu.matmul_pop(one)
        push(0, 0, 0)

        def trip(b, total):
            for step in range(total_steps):
                multiply(b * per + step // quads, step % quads, step % 2, step % ranges)
                push(b * per + (step + 1) // quads, (step + 1) % quads, (step + 1) % 2)
                if step < lag:
                    total = finish(b - 1, total_steps + step - lag, total)
                else:
                    total = finish(b, step - lag, total)
            return total

        trips = lax.div(count + per - 1, per)
        total = lax.fori_loop(0, trips, trip, jnp.zeros((8, width), jnp.float32))
        for step in range(total_steps - lag, total_steps):
            total = finish(trips - 1, step, total)
        for x in range(2):
            pltpu.matmul_acc_lhs(acc[x][0][0], jnp.zeros((width, 2 * width), jnp.bfloat16), load_staged_rhs=0)
            pltpu.matmul_pop(acc[x][0][0])

    pl.run_scoped(run, *[pltpu.ACC(x)((width, 2 * width), jnp.float32) for x in range(2) for _ in range(2 * ranges)])


def reduce_kernel(n, groups, slots, teams, occupied, fixed, batch, listed, counts, singles, occ, vir, integrals_ref, dp_ref, cp_ref, row_ref,
                  part_ref, trip_ref, mean_ref, all_buf, send_sem, recv_sem, own_ref, vbc_ref):
    g = lax.axis_index("grp")
    q = lax.axis_index("blk")
    barrier = pltpu.get_barrier_semaphore()
    others = [(dg, dq) for dg in range(groups) for dq in range(n) if dg or dq]
    for dg, dq in others:
        pl.semaphore_signal(barrier, inc=1, device_id={"grp": (g + dg) % groups, "blk": (q + dq) % n}, device_id_type=MESH)

    blocks, width = integrals_ref.shape[1], integrals_ref.shape[2]
    first = (g % 2) * blocks
    across = jnp.broadcast_to(row_ref[...], (width, width))
    vbc_ref[...] = across + across.T
    count = counts[0, 0]
    spots = lax.broadcasted_iota(jnp.int32, part_ref.shape, 0) * part_ref.shape[1] + lax.broadcasted_iota(jnp.int32, part_ref.shape, 1)
    contract = (((1,), (1,)), ((), ()))

    def step(b, table):
        for u in range(batch):
            at = b * batch + u
            code = listed[0, at]
            k = lax.rem(code, occupied)
            j = lax.rem(lax.div(code, occupied), occupied)
            i = lax.rem(lax.div(code, occupied * occupied), occupied)
            place = lax.div(code, occupied * occupied * occupied)
            jk = lax.div(j * occupied + k, teams)
            kj = lax.div(k * occupied + j, teams)
            occ_sum = occ[i] + occ[j] + occ[k]
            d_jk, d_kj = dp_ref[jk], dp_ref[kj]
            total = jnp.zeros((8, width), jnp.float32)
            for a in range(blocks):
                block = integrals_ref[i, a]
                left = jnp.concatenate([block, d_jk], axis=1)
                right = jnp.concatenate([d_kj, block], axis=1)
                connected = lax.dot_general(left, right, contract, preferred_element_type=jnp.float32)
                full = connected + singles[i, first + a] * cp_ref[jk].astype(jnp.float32)
                denominator = (occ_sum - vir[q * 2 * blocks + first + a]) - vbc_ref[...]
                value = full * full / denominator
                total = total + jnp.sum(value.reshape(width // 8, 8, width), axis=0)
            here = jnp.logical_and(spots == place, at < count)
            table = table + jnp.where(here, jnp.sum(total), 0.0)
        return table

    own_ref[...] = lax.fori_loop(0, fixed // batch, step, part_ref[...])
    pl.semaphore_wait(barrier, len(others))
    copies = []
    for at, (dg, dq) in enumerate(others):
        copy = pltpu.make_async_remote_copy(
            src_ref=own_ref, dst_ref=all_buf.at[g * n + q], send_sem=send_sem.at[at], recv_sem=recv_sem.at[at],
            device_id={"grp": (g + dg) % groups, "blk": (q + dq) % n}, device_id_type=MESH)
        copy.start()
        copies.append(copy)
    all_buf[g * n + q] = own_ref[...]
    for copy in copies:
        copy.wait()
    table = jnp.sum(all_buf[...], axis=0)
    spread = lax.broadcasted_iota(jnp.int32, (slots, table.shape[1]), 1) - lax.broadcasted_iota(jnp.int32, (slots, table.shape[1]), 0)
    shown = jnp.zeros((slots, table.shape[1]), jnp.float32)
    for line in range(table.shape[0]):
        shown += jnp.where(spread == g * slots - line * table.shape[1], table[line:line + 1], 0.0)
    trip_ref[...] = jnp.sum(shown, axis=1)[None, :]
    mean_ref[...] = jnp.sum(table, keepdims=True) / (groups * slots)


def body(n, groups, integrals, doubles, coulomb, singles, occ_energy, vir_energy, triplets, tile_count):
    occupied, _, width, _ = integrals.shape
    rows = doubles.shape[0]
    slots = triplets.shape[1]
    teams = team_count(occupied, rows, groups)
    runs = rows // teams
    pairs = n * runs
    f32, i32 = jnp.float32, jnp.int32
    vmem = pl.BlockSpec(memory_space=pltpu.VMEM)
    smem = pl.BlockSpec(memory_space=pltpu.SMEM)
    hbm = pl.BlockSpec(memory_space=pltpu.HBM)
    dma = pltpu.SemaphoreType.DMA

    row_bytes = pairs * width * width * doubles.dtype.itemsize
    spare = 1 << 20
    blocks = integrals.shape[1] // 2
    half = jax.ShapeDtypeStruct((occupied, blocks, width, width), integrals.dtype)
    keep = half.size * half.dtype.itemsize + 4 * row_bytes + 2 * spare
    lanes = -(-slots // 128) * 128
    length = -(-groups * slots // 128) * 128
    fixed, batch = 8, 8
    sheet = (-(-groups * slots // 128), 128)

    packed = jax.ShapeDtypeStruct((pairs, width, width), doubles.dtype)
    dp, cp, held, listed, counts = pl.pallas_call(
        functools.partial(gather_kernel, n, groups, teams, occupied, slots),
        out_shape=(packed, packed, half, jax.ShapeDtypeStruct((1, length), i32), jax.ShapeDtypeStruct((1, 128), i32)),
        in_specs=[hbm] * 4 + [pl.BlockSpec(memory_space=pl.ANY)],
        out_specs=(vmem, vmem, vmem, vmem, vmem),
        scratch_shapes=[
            pltpu.VMEM((groups, 1, lanes), i32), pltpu.VMEM((3, 1, slots), i32), pltpu.VMEM((1, 1), i32), dma((2,)), dma, dma((runs, 2)),
            dma((runs, 2, n - 1)), dma((runs, 2, n - 1)), dma((runs, 2, n - 1)), dma((runs, 2, n - 1)),
            dma((2, groups // 2)), dma((2, groups // 2)), dma((groups,)), dma((groups,)), pltpu.SemaphoreType.REGULAR((2, groups // 2)),
        ],
        compiler_params=pltpu.CompilerParams(collective_id=0, has_side_effects=True, vmem_limit_bytes=keep),
        name="gather",
    )(*(pltpu.with_memory_space_constraint(x, pltpu.HBM)
        for x in (doubles, coulomb, integrals, jnp.transpose(triplets, (2, 0, 1)))), tile_count.reshape(1, 1))

    part = pl.pallas_call(
        functools.partial(compute_kernel, groups, slots, teams, occupied, fixed),
        out_shape=jax.ShapeDtypeStruct(sheet, f32),
        in_specs=[smem, smem, smem, smem, smem, vmem, vmem, vmem, vmem],
        out_specs=vmem,
        scratch_shapes=[pltpu.VMEM((width, width), f32), pltpu.VMEM((pairs, width, width), f32)],
        compiler_params=pltpu.CompilerParams(vmem_limit_bytes=keep),
        name="energy",
    )(listed, counts, singles, occ_energy, vir_energy, held, dp, cp, vir_energy.reshape(1, width))

    trip, mean = pl.pallas_call(
        functools.partial(reduce_kernel, n, groups, slots, teams, occupied, fixed, batch),
        out_shape=(jax.ShapeDtypeStruct((1, slots), f32), jax.ShapeDtypeStruct((1, 1), f32)),
        in_specs=[smem, smem, smem, smem, smem, vmem, vmem, vmem, vmem, vmem],
        out_specs=(vmem, vmem),
        scratch_shapes=[
            pltpu.VMEM((groups * n, *sheet), f32), dma((groups * n - 1,)), dma((groups * n - 1,)), pltpu.VMEM(sheet, f32), pltpu.VMEM((width, width), f32),
        ],
        compiler_params=pltpu.CompilerParams(collective_id=1, has_side_effects=True, vmem_limit_bytes=keep),
        name="join",
    )(listed, counts, singles, occ_energy, vir_energy, held, dp, cp, vir_energy.reshape(1, width), part)
    return trip, mean.reshape(())


def solution(mesh):
    in_specs = (
        P(None, "blk", None, None),
        P("blk", None, None),
        P("blk", None, None),
        P(None, "blk"),
        P(),
        P(),
        P("grp", None, None),
        P("grp"),
    )
    out_specs = (P("grp", None), P())
    step = functools.partial(body, mesh.shape["blk"], mesh.shape["grp"])
    return jax.shard_map(step, mesh=mesh, in_specs=in_specs, out_specs=out_specs, check_vma=False)
```
